128 devices in a mesh: grp: 4 (over z), dev: 32 (over x, y, core).
Axes of the slice: x: 4, y: 4, z: 4, core: 2. Of those that a mesh axis runs over, the one named last changes fastest.
Arguments:
- matrix_tiles: bfloat16 [10240, 128, 1024], P(('grp', 'dev')), may hold values from -0.125 to 0.125
- tile_column: int32 [10240], P(('grp', 'dev')), may hold values from 0 to 255
- block_counts: int32 [4096], P(('grp', 'dev')), may hold values from 1 to 4, as said below
- destination: int32 [4096], P(('grp', 'dev')), may hold values from 0 to 31, as said below
- row_bounds: bfloat16 [524288], P(('grp', 'dev')), may hold values from -6 to 6
- dual_start: bfloat16 [524288], P(('grp', 'dev')), may hold values from 0 to 1
- primal_start: float32 [262144], replicated, may hold values from 0 to 0.5
- cost_vector: float32 [262144], replicated, may hold values from -6 to 6
- upper_bound: float32 [262144], replicated, may hold values from 0.5 to 2
Outputs:
- primal_final: float32 [262144], replicated
- dual_final: float32 [524288], P(('grp', 'dev'))
- weight_final: float32 [1], replicated
The draws below stay inside these ranges and needn't reach their ends.
Inputs may be any that keep to these rules, and one draw needn't show every extreme that they name: `block_counts`: each device's 32 row blocks have 1 to 4 tiles each and 80 at most together; some device has exactly 80 in every draw. `destination`: on every device the 32 entries are each of 0 to 31 once.
All inputs are finite; a program needn't handle non-finite values.
Results may differ from the reference program's by a relative error of at most 0.0015.
Values may be sent and summed in bfloat16 or wider, within the bound.
A program may use at most 128 MiB of HBM per device.

```python
import jax
import jax.numpy as jnp
from jax import lax

CB = 1024
NCB = 256
TR = 128
MAXC = 4
ITERS = 3
RB_DEV = 32
POOL_DEV = 80
RBLK = 4096
ROWS = 524288
COLS = 262144
N_GRP = 4
N_DEV = 32


def layout_pair(key):
    device_count = RBLK // RB_DEV
    base_key = jax.random.fold_in(key, 7)
    key_extra, key_heavy, key_rank, key_tie = jax.random.split(base_key, 4)
    extra_tiles = jax.random.randint(key_extra, (device_count,), 0, POOL_DEV - RB_DEV + 1)
    heaviest = jax.random.randint(key_heavy, (), 0, device_count)
    extra_tiles = jnp.where(jnp.arange(device_count) == heaviest, POOL_DEV - RB_DEV, extra_tiles)
    rank_of = jax.vmap(lambda sub: jax.random.permutation(sub, RB_DEV))(jax.random.split(key_rank, device_count))
    counts = 1 + jnp.clip(extra_tiles[:, None] - rank_of * (MAXC - 1), 0, MAXC - 1)
    tie_break = jax.vmap(lambda sub: jax.random.permutation(sub, RB_DEV))(jax.random.split(key_tie, device_count))
    sorted_slots = jnp.argsort(counts * RB_DEV + tie_break, axis=1)
    position = jnp.argsort(sorted_slots, axis=1)
    member = (jnp.arange(device_count) % RB_DEV)[:, None]
    target_dev = (position + member) % RB_DEV
    return (counts.astype(jnp.int32).reshape(RBLK), target_dev.astype(jnp.int32).reshape(RBLK))


def draw_block_counts(key, part):
    return layout_pair(key)[0]


def draw_destination(key, part):
    return layout_pair(key)[1]


def plant(result, rng, low, top_value):
    longest = result.shape.index(max(result.shape))
    spots = []
    for shift in (0, 1):
        where = [jax.random.randint(jax.random.fold_in(rng, axis), (), 0, length) for axis, length in enumerate(result.shape)]
        where[longest] = (where[longest] + shift) % result.shape[longest]
        spots.append(tuple(where))
    return result.at[spots[0]].set(low).at[spots[1]].set(top_value)


def steps_of(own_key, extent, shards, low, top_value):
    level = 1.0
    for dim, blocks in shards:
        heights = jax.random.uniform(jax.random.fold_in(jax.random.fold_in(own_key, 6), dim), (blocks,), jnp.float32, low / len(shards), top_value / len(shards))
        level = level * jnp.repeat(jnp.exp(heights), extent[dim] // blocks).reshape((-1,) + (1,) * (len(extent) - 1 - dim))
    return level


def bell_draw(own_key, shape, spread, reach, cuts=(), kind=jnp.bfloat16):
    gain = steps_of(own_key, shape, cuts, -0.22, 0.18) if cuts else 1.0
    drawn = jax.random.normal(own_key, shape, jnp.float32) * spread * gain
    return jnp.minimum(jnp.maximum(drawn, -reach), reach).astype(kind)


def setup_inputs(seed: int = 0) -> dict:
    key_list = jax.random.split(jax.random.key(seed), 10)
    matrix_tiles = bell_draw(key_list[0], (N_GRP * N_DEV * POOL_DEV, TR, CB), (2 * CB) ** -0.5, 0.125, ((0, 128),))
    tile_column = plant(jax.random.randint(key_list[1], (N_GRP * N_DEV * POOL_DEV,), 0, NCB), jax.random.fold_in(key_list[1], 1), 0, NCB - 1).astype(jnp.int32)
    block_counts = draw_block_counts(jax.random.fold_in(key_list[9], 71), 0)
    destination = draw_destination(jax.random.fold_in(key_list[9], 71), 0)
    row_bounds = bell_draw(key_list[4], (ROWS,), 1.0, 6.0, ((0, 128),))
    dual_start = jnp.clip(1.0 * jax.random.uniform(key_list[5], (ROWS,), jnp.float32) ** steps_of(key_list[5], (ROWS,), ((0, 128),), -0.2, 0.2), 0.0, 1.0).astype(jnp.bfloat16)
    primal_start = jnp.clip(jax.random.uniform(key_list[6], (COLS,), jnp.float32, 0.0, 0.5), 0.0, 0.5)
    cost_vector = bell_draw(key_list[7], (COLS,), 1.0, 6.0, (), jnp.float32)
    upper_bound = jnp.clip(jax.random.uniform(key_list[8], (COLS,), jnp.float32, 0.5, 2.0), 0.5, 2.0)
    return {"matrix_tiles": matrix_tiles, "tile_column": tile_column, "block_counts": block_counts, "destination": destination, "row_bounds": row_bounds, "dual_start": dual_start, "primal_start": primal_start, "cost_vector": cost_vector, "upper_bound": upper_bound}


step_scale = 0.3

def reference(matrix_tiles, tile_column, block_counts, destination, row_bounds, dual_start, primal_start, cost_vector, upper_bound):
    device_count = N_GRP * N_DEV
    tile_set = matrix_tiles.reshape(device_count, POOL_DEV, TR, CB)
    tile_cols = tile_column.reshape(device_count, POOL_DEV)
    counts = block_counts.reshape(device_count, RB_DEV)
    starts = jnp.cumsum(counts, axis=1) - counts
    slot_ids = jnp.arange(POOL_DEV, dtype=jnp.int32)
    owners = lax.optimization_barrier(jnp.sum((starts[:, None, 1:] <= slot_ids[None, :, None]).astype(jnp.int32), axis=2))
    is_live = slot_ids[None, :] < lax.optimization_barrier(jnp.sum(counts, axis=1))[:, None]

    def apply_rows(vector_bf):
        vector_table = vector_bf.astype(jnp.float32).reshape(NCB, CB)

        def per_device(entries):
            tile_d, col_d, own_d, live_d = entries
            product = jnp.einsum('src,sc->sr', tile_d.astype(jnp.float32), vector_table[col_d], precision=lax.Precision.HIGHEST)
            product = jnp.where(live_d[:, None], product, 0.0)
            return jax.ops.segment_sum(product, own_d, num_segments=RB_DEV)
        return lax.map(per_device, (tile_set, tile_cols, owners, is_live))

    def apply_columns(rows_bf):

        def per_device(accum, entries):
            tile_d, col_d, own_d, live_d, rows_d = entries
            product = jnp.einsum('src,sr->sc', tile_d.astype(jnp.float32), rows_d.astype(jnp.float32)[own_d], precision=lax.Precision.HIGHEST)
            product = jnp.where(live_d[:, None], product, 0.0)
            return (accum + jax.ops.segment_sum(product, col_d, num_segments=NCB), None)
        accum, unused = lax.scan(per_device, jnp.zeros((NCB, CB), jnp.float32), (tile_set, tile_cols, owners, is_live, rows_bf))
        return accum.reshape(-1)
    bounds = row_bounds.astype(jnp.float32).reshape(device_count, RB_DEV, TR)
    dual_state = dual_start.astype(jnp.float32).reshape(device_count, RB_DEV, TR)
    primal = primal_start
    weight = jnp.ones((), jnp.float32)
    row_image = apply_rows(primal.astype(jnp.bfloat16))
    for iteration in range(ITERS):
        step_primal = step_scale / weight
        step_dual = step_scale * weight
        gradient = apply_columns(dual_state.astype(jnp.bfloat16))
        primal_next = jnp.clip(primal - step_primal * (cost_vector - gradient), 0.0, upper_bound)
        change = jnp.sum((primal_next - primal) ** 2)
        next_image = apply_rows(primal_next.astype(jnp.bfloat16))
        dual_state = jnp.maximum(dual_state + step_dual * (bounds - (2.0 * next_image - row_image)), 0.0)
        violation = jnp.sum(jnp.maximum(bounds - next_image, 0.0) ** 2)
        weight = jnp.sqrt(weight * jnp.sqrt((violation + 1e-06) / (change + 1e-06)))
        primal = primal_next
        row_image = next_image
    grouped = dual_state.reshape(N_GRP, N_DEV, RB_DEV, TR)
    target = destination.reshape(N_GRP, N_DEV, RB_DEV)
    group_index = jnp.broadcast_to(jnp.arange(N_GRP, dtype=jnp.int32)[:, None, None], target.shape)
    member_index = jnp.broadcast_to(jnp.arange(N_DEV, dtype=jnp.int32)[None, :, None], target.shape)
    placed = jnp.zeros((N_GRP, N_DEV, N_DEV, TR), jnp.float32).at[group_index, target, member_index].set(grouped)
    return (primal, placed.reshape(-1), jnp.reshape(weight, (1,)))
```

```python
import jax
import jax.numpy as jnp
from jax import lax
from jax.experimental import pallas as pl
from jax.experimental.pallas import tpu as pltpu
from jax.sharding import PartitionSpec as P

MESH = pl.DeviceIdType.MESH
GRP_DEV = ("grp", "dev")

NCB = 256
CB = 1024
TR = 128
SLOTS = 80
BLOCKS = 32
ITERS = 3
CH = 4
LANES = CB // CH
GROUP = 16
NG = SLOTS // GROUP
PLANE = 32
ZN = 4
STEP = 0.3

F32 = jnp.float32
BF16 = jnp.bfloat16


def iota(shape, dim):
    return lax.broadcasted_iota(jnp.int32, shape, dim)


def dot(a, b, dims=((1,), (0,)), exact=False):
    return lax.dot_general(
        a,
        b,
        (dims, ((), ())),
        precision=lax.Precision.HIGHEST if exact else None,
        preferred_element_type=F32,
    )


def kernel(
    tiles_hbm,
    col_ref,
    cnt_ref,
    dst_ref,
    bnd_ref,
    dual0_ref,
    x_hbm,
    c_hbm,
    u_hbm,
    xo_ref,
    do_ref,
    wo_ref,
    tiles,
    x,
    cost,
    upper,
    xtab,
    cmat,
    ctmat,
    omat,
    otmat,
    bd,
    prod,
    macc,
    vsel,
    img,
    dual,
    wgt,
    snd,
    rcv,
    zsnd,
    zrcv,
    grad,
    vsnd,
    vrcv,
    vzsnd,
    vzrcv,
    dsnd,
    drcv,
    bounds,
    tile_sem,
    vec_sem,
    out_sem,
    snd_sem,
    rcv_sem,
    zsnd_sem,
    zrcv_sem,
    gzs_sem,
    gzr_sem,
    gs_sem,
    gr_sem,
    vs_sem,
    vr_sem,
    vzs_sem,
    vzr_sem,
    ds_sem,
    dr_sem,
):
    z = lax.axis_index("grp")
    me = lax.axis_index("dev")

    vec_copies = [
        pltpu.make_async_copy(h, v, vec_sem.at[n])
        for n, (h, v) in enumerate(((x_hbm, x), (c_hbm, cost), (u_hbm, upper)))
    ]
    vec_copies[0].start()

    def tile_copy(j):
        return pltpu.make_async_copy(
            tiles_hbm.at[:, :, pl.ds(LANES * j, LANES)], tiles.at[j], tile_sem.at[j]
        )

    for j in range(CH):
        tile_copy(j).start()
    vec_copies[1].start()
    vec_copies[2].start()

    barrier = pltpu.get_barrier_semaphore()

    def greet(k, _):
        pl.semaphore_signal(
            barrier, inc=1, device_id=(z, lax.rem(me + k, PLANE)), device_id_type=MESH
        )
        return 0

    lax.fori_loop(1, PLANE, greet, 0)
    for k in range(1, ZN):
        pl.semaphore_signal(
            barrier, inc=1, device_id=(lax.rem(z + k, ZN), me), device_id_type=MESH
        )

    def to_plane(src, dst, ssem, rsem):
        def go(k, _):
            peer = lax.rem(me + k, PLANE)
            pltpu.make_async_remote_copy(
                src_ref=src(peer),
                dst_ref=dst,
                send_sem=ssem,
                recv_sem=rsem,
                device_id=(z, peer),
                device_id_type=MESH,
            ).start()
            return 0

        lax.fori_loop(1, PLANE, go, 0)

    def to_z(src, dst, ssem, rsem, peer_z):
        pltpu.make_async_remote_copy(
            src_ref=src,
            dst_ref=dst,
            send_sem=ssem,
            recv_sem=rsem,
            device_id=(peer_z, me),
            device_id_type=MESH,
        ).start()

    def await_bytes(ref, sem):
        pltpu.make_async_copy(ref, ref, sem).wait()

    cols = jnp.broadcast_to(col_ref[...], (NCB, SLOTS))
    onehot = (cols == iota((NCB, SLOTS), 0)).astype(F32)
    onehot = jnp.concatenate([onehot, jnp.zeros((NCB, TR - SLOTS), F32)], axis=1)
    cmat[...] = onehot.astype(BF16)
    ctmat[...] = onehot.T.astype(BF16)
    counts = jnp.broadcast_to(cnt_ref[...], (TR, BLOCKS)).astype(F32)
    below = (iota((BLOCKS, BLOCKS), 1) < iota((BLOCKS, BLOCKS), 0)).astype(F32)
    upto = (iota((BLOCKS, BLOCKS), 1) <= iota((BLOCKS, BLOCKS), 0)).astype(F32)
    starts = dot(below, counts, ((1,), (1,)))
    ends = dot(upto, counts, ((1,), (1,)))
    slot = iota((BLOCKS, TR), 1).astype(F32)
    owner = jnp.where((starts <= slot) & (slot < ends), 1.0, 0.0)
    omat[...] = owner
    owner = jnp.concatenate([owner, jnp.zeros((TR - BLOCKS, TR), F32)], axis=0)
    otmat[...] = owner.T.astype(BF16)
    prod[...] = jnp.zeros_like(prod)
    macc[...] = jnp.zeros_like(macc)
    wgt[...] = jnp.ones_like(wgt)
    dual[...] = jnp.zeros_like(dual)
    dual[pl.ds(0, BLOCKS), :] = dual0_ref[...].astype(F32)
    bounds[...] = bnd_ref[...].astype(F32)

    def pieces(j, body, start):
        def row(p, carry):
            for c in range(2):
                at = pl.ds(TR * p + 2 * j + c, 16, stride=8)
                carry = body(p, c, at, carry)
            return carry

        return lax.fori_loop(0, 16, row, start)

    def table(j, p, c, value):
        xtab[j, pl.ds(pl.multiple_of(16 * p, 16), 16), pl.ds(TR * c, TR)] = value.astype(BF16)

    vec_copies[0].wait()
    for j in range(CH):

        def first_table(p, c, at, carry, j=j):
            table(j, p, c, x[at, :])
            return carry

        pieces(j, first_table, 0)

    def columns(it, j):
        def group(g, _):
            rows = pl.ds(pl.multiple_of(GROUP * g, GROUP), GROUP)
            block = tiles[j, rows].reshape(GROUP * TR, LANES)
            prod[rows, :] = dot(bd[g], block)
            return 0

        lax.fori_loop(0, NG, group, 0)
        full = prod[...]
        high = full.astype(BF16)
        low = (full - high.astype(F32)).astype(BF16)
        total = dot(cmat[...], high) + dot(cmat[...], low)
        total = total.astype(BF16)
        for c in range(2):
            snd[it, j, pl.ds(16 * c, 16)] = total[:, TR * c : TR * (c + 1)].reshape(16, 16, TR)
        to_plane(lambda i: snd.at[it, j, i], rcv.at[it, j, me], snd_sem.at[it, j], rcv_sem.at[it, j])

    def rows(j):
        vsel[...] = dot(ctmat[...], xtab[j]).astype(BF16)
        lane = iota((TR, TR), 1)

        def group(g, merged):
            at = pl.ds(pl.multiple_of(GROUP * g, GROUP), GROUP)
            block = tiles[j, at].reshape(GROUP * TR, LANES)
            out = dot(block, vsel[...], ((1,), (1,)))
            for k in range(GROUP):
                merged = jnp.where(lane == GROUP * g + k, out[TR * k : TR * (k + 1)], merged)
            return merged

        macc[...] += lax.fori_loop(0, NG, group, jnp.zeros((TR, TR), F32))

    def rows_done():
        out = dot(omat[...], macc[...], ((1,), (1,)), exact=True)
        macc[...] = jnp.zeros_like(macc)
        return out

    def plane_sum(it, j):
        rcv[it, j, me] = snd[it, j, me]
        await_bytes(rcv.at[it, j, pl.ds(0, PLANE - 1)], rcv_sem.at[it, j])
        total = rcv[it, j, 0].astype(F32)
        for i in range(1, PLANE):
            total += rcv[it, j, i].astype(F32)

        @pl.when(z == j)
        def _():
            zrcv[it, j] = total

        @pl.when(z != j)
        def _():
            zsnd[it, j] = total
            to_z(zsnd.at[it, j], zrcv.at[it, z], zsnd_sem.at[it, j], zrcv_sem.at[it], j)

    def root_sum(it, j):
        @pl.when(z == j)
        def _():
            await_bytes(zrcv.at[it, pl.ds(0, ZN - 1)], zrcv_sem.at[it])
            total = zrcv[it, 0] + zrcv[it, 1] + zrcv[it, 2] + zrcv[it, 3]
            grad[it, j, me] = total.astype(BF16)
            for k in range(1, ZN):
                to_z(
                    grad.at[it, j, me],
                    grad.at[it, j, me],
                    gzs_sem.at[it],
                    gzr_sem.at[it, j],
                    lax.rem(z + k, ZN),
                )

    def spread(it, j):
        @pl.when(z != j)
        def _():
            await_bytes(grad.at[it, j, me], gzr_sem.at[it, j])

        to_plane(
            lambda i: grad.at[it, j, me], grad.at[it, j, me], gs_sem.at[it, j], gr_sem.at[it, j]
        )

    def violation_out(it, violated):
        part = violated[0:8] + violated[8:16] + violated[16:24] + violated[24:32]
        part = jnp.sum(part, axis=0, keepdims=True)
        vsnd[it] = part
        vrcv[it, me] = part
        to_plane(lambda i: vsnd.at[it], vrcv.at[it, me], vs_sem.at[it], vr_sem.at[it])

    def violation_plane(it):
        await_bytes(vrcv.at[it, pl.ds(0, PLANE - 1)], vr_sem.at[it])
        total = vrcv[it, 0]
        for i in range(1, PLANE):
            total += vrcv[it, i]
        vzsnd[it] = total
        vzrcv[it, z] = total
        for k in range(1, ZN):
            to_z(
                vzsnd.at[it],
                vzrcv.at[it, z],
                vzs_sem.at[it],
                vzr_sem.at[it],
                lax.rem(z + k, ZN),
            )

    def new_weight(it):
        await_bytes(vzrcv.at[it, pl.ds(0, ZN - 1)], vzr_sem.at[it])
        total = vzrcv[it, 0] + vzrcv[it, 1] + vzrcv[it, 2] + vzrcv[it, 3]
        violation = jnp.sum(total, axis=1, keepdims=True)
        change = wgt[pl.ds(8, 8), :]
        ratio = (jnp.broadcast_to(violation, (8, TR)) + 1e-6) / (change + 1e-6)
        wgt[pl.ds(0, 8), :] = jnp.sqrt(wgt[pl.ds(0, 8), :] * jnp.sqrt(ratio))

    def update(it, j, tau, moved):
        def piece(p, c, at, carry):
            old = x[at, :]
            slope = grad[it, j, 16 * c + p].astype(F32)
            new = jnp.minimum(jnp.maximum(old - tau * (cost[at, :] - slope), 0.0), upper[at, :])
            x[at, :] = new
            table(j, p, c, new)
            return carry + (new - old) * (new - old)

        return pieces(j, piece, moved)

    def iteration(it, _):
        chosen = dot(otmat[...], dual[...].astype(BF16))
        line = iota((GROUP, TR), 0)
        for g in range(NG):
            part = chosen[GROUP * g : GROUP * (g + 1)]
            for k in range(GROUP):
                bd[g, :, pl.ds(TR * k, TR)] = jnp.where(line == k, part, 0.0).astype(BF16)
        for j in range(CH):

            @pl.when(it == 0)
            def _():
                tile_copy(j).wait()
                if j == 0:
                    pl.semaphore_wait(barrier, PLANE - 1 + ZN - 1)

            columns(it, j)

        def early_rows(j):
            @pl.when(it == 0)
            def _():
                rows(j)

        plane_sum(it, 0)
        plane_sum(it, 1)
        root_sum(it, 0)
        plane_sum(it, 2)
        root_sum(it, 1)
        plane_sum(it, 3)
        early_rows(0)
        spread(it, 0)
        root_sum(it, 2)
        spread(it, 1)
        root_sum(it, 3)
        early_rows(1)

        @pl.when(it > 0)
        def _():
            violation_plane(it - 1)

        spread(it, 2)
        spread(it, 3)
        early_rows(2)
        early_rows(3)

        @pl.when(it == 0)
        def _():
            img[...] = rows_done()
            vec_copies[1].wait()
            vec_copies[2].wait()

        @pl.when(it > 0)
        def _():
            new_weight(it - 1)

        weight = wgt[pl.ds(0, 1), :]
        tau = STEP / weight
        sigma = STEP * weight
        moved = jnp.zeros((16, TR), F32)
        for j in range(CH):
            grad_at = grad.at[it, j, pl.ds(0, PLANE - 1)]
            await_bytes(grad_at, gr_sem.at[it, j])
            moved = update(it, j, tau, moved)
            rows(j)

        @pl.when(it == ITERS - 1)
        def _():
            pltpu.make_async_copy(x, xo_ref, out_sem).start()

        change = jnp.sum(jnp.sum(moved, axis=0, keepdims=True), axis=1, keepdims=True)
        wgt[pl.ds(8, 8), :] = jnp.broadcast_to(change, (8, TR))
        image = rows_done()
        violated = jnp.maximum(bounds[...] - image, 0.0)
        violation_out(it, violated * violated)
        dual[pl.ds(0, BLOCKS), :] = jnp.maximum(
            dual[pl.ds(0, BLOCKS), :] + sigma * (bounds[...] - (2.0 * image - img[...])), 0.0
        )
        img[...] = image
        return 0

    lax.fori_loop(0, ITERS, iteration, 0)

    hot = jnp.broadcast_to(dst_ref[...], (BLOCKS, BLOCKS)) == iota((BLOCKS, BLOCKS), 0)
    ordered = dot(hot.astype(F32), dual[pl.ds(0, BLOCKS), :], exact=True)
    for i in range(BLOCKS):
        dsnd[i] = ordered[i : i + 1]
    drcv[me] = dsnd[me]
    to_plane(lambda i: dsnd.at[i], drcv.at[me], ds_sem, dr_sem)
    violation_plane(ITERS - 1)
    await_bytes(drcv.at[pl.ds(0, PLANE - 1)], dr_sem)
    do_ref[...] = drcv[...]
    new_weight(ITERS - 1)
    wo_ref[...] = wgt[pl.ds(0, 8), :]

    def drain(it, _):
        for j in range(CH):
            await_bytes(snd.at[it, j, pl.ds(0, PLANE - 1)], snd_sem.at[it, j])
            await_bytes(grad.at[it, j, pl.ds(0, PLANE - 1)], gs_sem.at[it, j])

            @pl.when(z != j)
            def _():
                await_bytes(zsnd.at[it, j], zsnd_sem.at[it, j])

        await_bytes(grad.at[it, 0, pl.ds(0, ZN - 1)], gzs_sem.at[it])
        await_bytes(vrcv.at[it, pl.ds(0, PLANE - 1)], vs_sem.at[it])
        await_bytes(vzrcv.at[it, pl.ds(0, ZN - 1)], vzs_sem.at[it])
        return 0

    lax.fori_loop(0, ITERS, drain, 0)
    await_bytes(dsnd.at[pl.ds(0, PLANE - 1)], ds_sem)
    pltpu.make_async_copy(x, xo_ref, out_sem).wait()


def per_device(tiles, col, counts, dest, bounds, dual0, primal, cost, upper):
    anywhere = pl.BlockSpec(memory_space=pl.ANY)
    vmem = pl.BlockSpec(memory_space=pltpu.VMEM)
    dma = pltpu.SemaphoreType.DMA
    flat = (NCB * CB // TR, TR)
    x_out, dual_out, weight = pl.pallas_call(
        kernel,
        out_shape=(
            jax.ShapeDtypeStruct(flat, F32),
            jax.ShapeDtypeStruct((BLOCKS, 1, TR), F32),
            jax.ShapeDtypeStruct((8, TR), F32),
        ),
        in_specs=[anywhere, vmem, vmem, vmem, vmem, vmem, anywhere, anywhere, anywhere],
        out_specs=(anywhere, vmem, vmem),
        scratch_shapes=[
            pltpu.VMEM((CH, SLOTS, TR, LANES), BF16),
            pltpu.VMEM(flat, F32),
            pltpu.VMEM(flat, F32),
            pltpu.VMEM(flat, F32),
            pltpu.VMEM((CH, NCB, LANES), BF16),
            pltpu.VMEM((NCB, TR), BF16),
            pltpu.VMEM((TR, NCB), BF16),
            pltpu.VMEM((BLOCKS, TR), F32),
            pltpu.VMEM((TR, TR), BF16),
            pltpu.VMEM((NG, GROUP, GROUP * TR), BF16),
            pltpu.VMEM((TR, LANES), F32),
            pltpu.VMEM((TR, TR), F32),
            pltpu.VMEM((TR, LANES), BF16),
            pltpu.VMEM((BLOCKS, TR), F32),
            pltpu.VMEM((TR, TR), F32),
            pltpu.VMEM((16, TR), F32),
            pltpu.VMEM((ITERS, CH, PLANE, 16, TR), BF16),
            pltpu.VMEM((ITERS, CH, PLANE, 16, TR), BF16),
            pltpu.VMEM((ITERS, CH, 16, TR), F32),
            pltpu.VMEM((ITERS, ZN, 16, TR), F32),
            pltpu.VMEM((ITERS, CH, PLANE, 16, TR), BF16),
            pltpu.VMEM((ITERS, 1, TR), F32),
            pltpu.VMEM((ITERS, PLANE, 1, TR), F32),
            pltpu.VMEM((ITERS, 1, TR), F32),
            pltpu.VMEM((ITERS, ZN, 1, TR), F32),
            pltpu.VMEM((BLOCKS, 1, TR), F32),
            pltpu.VMEM((BLOCKS, 1, TR), F32),
            pltpu.VMEM((BLOCKS, TR), F32),
            dma((CH,)),
            dma((3,)),
            dma,
            dma((ITERS, CH)),
            dma((ITERS, CH)),
            dma((ITERS, CH)),
            dma((ITERS,)),
            dma((ITERS,)),
            dma((ITERS, CH)),
            dma((ITERS, CH)),
            dma((ITERS, CH)),
            dma((ITERS,)),
            dma((ITERS,)),
            dma((ITERS,)),
            dma((ITERS,)),
            dma,
            dma,
        ],
        compiler_params=pltpu.CompilerParams(
            collective_id=0, has_side_effects=True, vmem_limit_bytes=60 * 1024 * 1024
        ),
    )(
        tiles,
        col.reshape(1, SLOTS),
        counts.reshape(1, BLOCKS),
        dest.reshape(1, BLOCKS),
        bounds.reshape(BLOCKS, TR),
        dual0.reshape(BLOCKS, TR),
        primal.reshape(flat),
        cost.reshape(flat),
        upper.reshape(flat),
    )
    return x_out.reshape(-1), dual_out.reshape(-1), weight[0, :1]


def solution(mesh):
    split, whole = P(GRP_DEV), P()
    return jax.shard_map(
        per_device,
        mesh=mesh,
        in_specs=(P(GRP_DEV, None, None), split, split, split, split, split, whole, whole, whole),
        out_specs=(whole, split, whole),
        check_vma=False,
    )
```

```python
import jax
import jax.numpy as jnp
from jax import lax
from jax.experimental import pallas as pl
from jax.experimental.pallas import tpu as pltpu
from jax.sharding import PartitionSpec as P

MESH = pl.DeviceIdType.MESH
GRP_DEV = ("grp", "dev")

NCB = 256
CB = 1024
TR = 128
SLOTS = 80
BLOCKS = 32
ITERS = 3
CH = 4
LANES = CB // CH
GROUP = 16
NG = SLOTS // GROUP
PLANE = 32
ZN = 4
STEP = 0.3

F32 = jnp.float32
BF16 = jnp.bfloat16


def iota(shape, dim):
    return lax.broadcasted_iota(jnp.int32, shape, dim)


def dot(a, b, dims=((1,), (0,)), exact=False):
    return lax.dot_general(
        a,
        b,
        (dims, ((), ())),
        precision=lax.Precision.HIGHEST if exact else None,
        preferred_element_type=F32,
    )


def kernel(
    tiles_hbm,
    col_ref,
    cnt_ref,
    dst_ref,
    bnd_ref,
    dual0_ref,
    x_hbm,
    c_hbm,
    u_hbm,
    xo_ref,
    do_ref,
    wo_ref,
    tiles,
    x,
    cost,
    upper,
    xtab,
    cmat,
    ctmat,
    omat,
    otmat,
    bd,
    prod,
    macc,
    vsel,
    img,
    dual,
    wgt,
    snd,
    rcv,
    zsnd,
    zrcv,
    grad,
    vsnd,
    vrcv,
    vzsnd,
    vzrcv,
    dsnd,
    drcv,
    bounds,
    tile_sem,
    vec_sem,
    out_sem,
    snd_sem,
    rcv_sem,
    zsnd_sem,
    zrcv_sem,
    gs_sem,
    gr_sem,
    vs_sem,
    vr_sem,
    vzs_sem,
    vzr_sem,
    ds_sem,
    dr_sem,
):
    z = lax.axis_index("grp")
    me = lax.axis_index("dev")

    vec_copies = [
        pltpu.make_async_copy(h, v, vec_sem.at[n])
        for n, (h, v) in enumerate(((x_hbm, x), (c_hbm, cost), (u_hbm, upper)))
    ]
    vec_copies[0].start()

    def tile_copy(j):
        return pltpu.make_async_copy(
            tiles_hbm.at[:, :, pl.ds(LANES * j, LANES)], tiles.at[j], tile_sem.at[j]
        )

    for j in range(CH):
        tile_copy(j).start()
    vec_copies[1].start()
    vec_copies[2].start()

    barrier = pltpu.get_barrier_semaphore()

    def greet(k, _):
        pl.semaphore_signal(
            barrier, inc=1, device_id=(z, lax.rem(me + k, PLANE)), device_id_type=MESH
        )
        return 0

    lax.fori_loop(1, PLANE, greet, 0)
    for k in range(1, ZN):
        pl.semaphore_signal(
            barrier, inc=1, device_id=(lax.rem(z + k, ZN), me), device_id_type=MESH
        )

    def to_plane(src, dst, ssem, rsem):
        for k in range(1, PLANE):
            peer = lax.rem(me + k, PLANE)
            pltpu.make_async_remote_copy(
                src_ref=src(peer),
                dst_ref=dst,
                send_sem=ssem,
                recv_sem=rsem,
                device_id=(z, peer),
                device_id_type=MESH,
            ).start()

    def to_z(src, dst, ssem, rsem, peer_z):
        pltpu.make_async_remote_copy(
            src_ref=src,
            dst_ref=dst,
            send_sem=ssem,
            recv_sem=rsem,
            device_id=(peer_z, me),
            device_id_type=MESH,
        ).start()

    def await_bytes(ref, sem):
        pltpu.make_async_copy(ref, ref, sem).wait()

    cols = jnp.broadcast_to(col_ref[...], (NCB, SLOTS))
    onehot = (cols == iota((NCB, SLOTS), 0)).astype(F32)
    onehot = jnp.concatenate([onehot, jnp.zeros((NCB, TR - SLOTS), F32)], axis=1)
    cmat[...] = onehot.astype(BF16)
    ctmat[...] = onehot.T.astype(BF16)
    counts = jnp.broadcast_to(cnt_ref[...], (TR, BLOCKS)).astype(F32)
    below = (iota((BLOCKS, BLOCKS), 1) < iota((BLOCKS, BLOCKS), 0)).astype(F32)
    upto = (iota((BLOCKS, BLOCKS), 1) <= iota((BLOCKS, BLOCKS), 0)).astype(F32)
    starts = dot(below, counts, ((1,), (1,)))
    ends = dot(upto, counts, ((1,), (1,)))
    slot = iota((BLOCKS, TR), 1).astype(F32)
    owner = jnp.where((starts <= slot) & (slot < ends), 1.0, 0.0)
    omat[...] = owner
    owner = jnp.concatenate([owner, jnp.zeros((TR - BLOCKS, TR), F32)], axis=0)
    otmat[...] = owner.T.astype(BF16)
    prod[...] = jnp.zeros_like(prod)
    macc[...] = jnp.zeros_like(macc)
    wgt[...] = jnp.ones_like(wgt)
    dual[...] = jnp.zeros_like(dual)
    dual[pl.ds(0, BLOCKS), :] = dual0_ref[...].astype(F32)
    bounds[...] = bnd_ref[...].astype(F32)

    def pieces(j, body, start):
        def row(p, carry):
            for c in range(2):
                at = pl.ds(TR * p + 2 * j + c, 16, stride=8)
                carry = body(p, c, at, carry)
            return carry

        return lax.fori_loop(0, 16, row, start, unroll=2)

    def table(j, p, c, value):
        xtab[j, pl.ds(pl.multiple_of(16 * p, 16), 16), pl.ds(TR * c, TR)] = value.astype(BF16)

    vec_copies[0].wait()
    for j in range(CH):

        def first_table(p, c, at, carry, j=j):
            table(j, p, c, x[at, :])
            return carry

        pieces(j, first_table, 0)

    def columns(it, j):
        def group(g, _):
            rows = pl.ds(pl.multiple_of(GROUP * g, GROUP), GROUP)
            block = tiles[j, rows].reshape(GROUP * TR, LANES)
            prod[rows, :] = dot(bd[g], block)
            return 0

        lax.fori_loop(0, NG, group, 0)
        full = prod[...]
        high = full.astype(BF16)
        low = (full - high.astype(F32)).astype(BF16)
        total = dot(cmat[...], high) + dot(cmat[...], low)
        total = total.astype(BF16)
        for c in range(2):
            snd[it, j, pl.ds(16 * c, 16)] = total[:, TR * c : TR * (c + 1)].reshape(16, 16, TR)

    def columns_out(it, j):
        to_plane(lambda i: snd.at[it, j, i], rcv.at[it, j, me], snd_sem.at[it, j], rcv_sem.at[it, j])

    def rows(j):
        vsel[...] = dot(ctmat[...], xtab[j]).astype(BF16)
        lane = iota((TR, TR), 1)

        def group(g, merged):
            block = tiles[j, pl.ds(GROUP * g, GROUP)].reshape(GROUP * TR, LANES)
            out = dot(block, vsel[...], ((1,), (1,)))
            for k in range(GROUP):
                merged = jnp.where(lane == GROUP * g + k, out[TR * k : TR * (k + 1)], merged)
            return merged

        merged = jnp.zeros((TR, TR), F32)
        for g in range(NG):
            merged = group(g, merged)
        macc[...] += merged

    def rows_done():
        out = dot(omat[...], macc[...], ((1,), (1,)), exact=True)
        macc[...] = jnp.zeros_like(macc)
        return out

    def plane_sum(it, j):
        rcv[it, j, me] = snd[it, j, me]
        await_bytes(rcv.at[it, j, pl.ds(0, PLANE - 1)], rcv_sem.at[it, j])
        total = rcv[it, j, 0].astype(F32)
        for i in range(1, PLANE):
            total += rcv[it, j, i].astype(F32)

        zsnd[it, j] = total
        zrcv[it, j, z] = total
        for k in range(1, ZN):
            to_z(
                zsnd.at[it, j],
                zrcv.at[it, j, z],
                zsnd_sem.at[it, j],
                zrcv_sem.at[it, j],
                lax.rem(z + k, ZN),
            )

    def spread(it, j):
        await_bytes(zrcv.at[it, j, pl.ds(0, ZN - 1)], zrcv_sem.at[it, j])
        total = zrcv[it, j, 0] + zrcv[it, j, 1] + zrcv[it, j, 2] + zrcv[it, j, 3]
        grad[it, j, me] = total.astype(BF16)
        to_plane(
            lambda i: grad.at[it, j, me], grad.at[it, j, me], gs_sem.at[it, j], gr_sem.at[it, j]
        )

    def violation_in(it, violated):
        part = violated[0:8] + violated[8:16] + violated[16:24] + violated[24:32]
        part = jnp.sum(part, axis=0, keepdims=True)
        vsnd[it] = part
        vrcv[it, me] = part

    def violation_out(it):
        to_plane(lambda i: vsnd.at[it], vrcv.at[it, me], vs_sem.at[it], vr_sem.at[it])

    def violation_plane(it):
        await_bytes(vrcv.at[it, pl.ds(0, PLANE - 1)], vr_sem.at[it])
        total = vrcv[it, 0]
        for i in range(1, PLANE):
            total += vrcv[it, i]
        vzsnd[it] = total
        vzrcv[it, z] = total
        for k in range(1, ZN):
            to_z(
                vzsnd.at[it],
                vzrcv.at[it, z],
                vzs_sem.at[it],
                vzr_sem.at[it],
                lax.rem(z + k, ZN),
            )

    def new_weight(it):
        await_bytes(vzrcv.at[it, pl.ds(0, ZN - 1)], vzr_sem.at[it])
        total = vzrcv[it, 0] + vzrcv[it, 1] + vzrcv[it, 2] + vzrcv[it, 3]
        violation = jnp.sum(total, axis=1, keepdims=True)
        change = wgt[pl.ds(8, 8), :]
        ratio = (jnp.broadcast_to(violation, (8, TR)) + 1e-6) / (change + 1e-6)
        wgt[pl.ds(0, 8), :] = jnp.sqrt(wgt[pl.ds(0, 8), :] * jnp.sqrt(ratio))

    def update(it, j, tau, moved):
        def piece(p, c, at, carry):
            old = x[at, :]
            slope = grad[it, j, 16 * c + p].astype(F32)
            new = jnp.minimum(jnp.maximum(old - tau * (cost[at, :] - slope), 0.0), upper[at, :])
            x[at, :] = new
            table(j, p, c, new)
            return carry + (new - old) * (new - old)

        return pieces(j, piece, moved)

    def iteration(it, _):
        chosen = dot(otmat[...], dual[...].astype(BF16))
        line = iota((GROUP, TR), 0)
        for g in range(NG):
            part = chosen[GROUP * g : GROUP * (g + 1)]
            for k in range(GROUP):
                bd[g, :, pl.ds(TR * k, TR)] = jnp.where(line == k, part, 0.0).astype(BF16)
        for j in range(CH):

            @pl.when(it == 0)
            def _():
                tile_copy(j).wait()

            columns(it, j)
            if j == 0:

                @pl.when(it == 0)
                def _():
                    pl.semaphore_wait(barrier, PLANE - 1 + ZN - 1)

            columns_out(it, j)
            if j == 0:

                @pl.when(it > 0)
                def _():
                    violation_out(it - 1)

        def early_rows(j):
            @pl.when(it == 0)
            def _():
                rows(j)

        plane_sum(it, 0)
        plane_sum(it, 1)
        early_rows(0)
        spread(it, 0)
        plane_sum(it, 2)
        early_rows(1)
        spread(it, 1)
        plane_sum(it, 3)
        early_rows(2)

        @pl.when(it > 0)
        def _():
            violation_plane(it - 1)

        spread(it, 2)
        early_rows(3)

        @pl.when(it == 0)
        def _():
            img[...] = rows_done()
            vec_copies[1].wait()
            vec_copies[2].wait()

        @pl.when(it > 0)
        def _():
            new_weight(it - 1)

        weight = wgt[pl.ds(0, 1), :]
        tau = STEP / weight
        sigma = STEP * weight
        moved = jnp.zeros((16, TR), F32)
        for j in range(CH):
            await_bytes(grad.at[it, j, pl.ds(0, PLANE - 1)], gr_sem.at[it, j])
            moved = update(it, j, tau, moved)
            if j == 0:
                spread(it, CH - 1)
            rows(j)

        @pl.when(it == ITERS - 1)
        def _():
            pltpu.make_async_copy(x, xo_ref, out_sem).start()

        change = jnp.sum(jnp.sum(moved, axis=0, keepdims=True), axis=1, keepdims=True)
        wgt[pl.ds(8, 8), :] = jnp.broadcast_to(change, (8, TR))
        image = rows_done()
        violated = jnp.maximum(bounds[...] - image, 0.0)
        violation_in(it, violated * violated)
        dual[pl.ds(0, BLOCKS), :] = jnp.maximum(
            dual[pl.ds(0, BLOCKS), :] + sigma * (bounds[...] - (2.0 * image - img[...])), 0.0
        )
        img[...] = image
        return 0

    lax.fori_loop(0, ITERS, iteration, 0)

    hot = jnp.broadcast_to(dst_ref[...], (BLOCKS, BLOCKS)) == iota((BLOCKS, BLOCKS), 0)
    ordered = dot(hot.astype(F32), dual[pl.ds(0, BLOCKS), :], exact=True)
    for i in range(BLOCKS):
        dsnd[i] = ordered[i : i + 1]
    drcv[me] = dsnd[me]
    violation_out(ITERS - 1)
    to_plane(lambda i: dsnd.at[i], drcv.at[me], ds_sem, dr_sem)
    violation_plane(ITERS - 1)
    await_bytes(drcv.at[pl.ds(0, PLANE - 1)], dr_sem)
    do_ref[...] = drcv[...]
    new_weight(ITERS - 1)
    wo_ref[...] = wgt[pl.ds(0, 8), :]

    def drain(it, _):
        for j in range(CH):
            await_bytes(snd.at[it, j, pl.ds(0, PLANE - 1)], snd_sem.at[it, j])
            await_bytes(grad.at[it, j, pl.ds(0, PLANE - 1)], gs_sem.at[it, j])
            await_bytes(zrcv.at[it, j, pl.ds(0, ZN - 1)], zsnd_sem.at[it, j])

        await_bytes(vrcv.at[it, pl.ds(0, PLANE - 1)], vs_sem.at[it])
        await_bytes(vzrcv.at[it, pl.ds(0, ZN - 1)], vzs_sem.at[it])
        return 0

    lax.fori_loop(0, ITERS, drain, 0)
    await_bytes(dsnd.at[pl.ds(0, PLANE - 1)], ds_sem)
    pltpu.make_async_copy(x, xo_ref, out_sem).wait()


def hand_over(x_ref, dual_ref, weight_ref, x_out, dual_out, weight_out):
    x_out[...] = x_ref[...]
    dual_out[...] = dual_ref[...]
    weight_out[0] = weight_ref[0, 0]


def per_device(tiles, col, counts, dest, bounds, dual0, primal, cost, upper):
    anywhere = pl.BlockSpec(memory_space=pl.ANY)
    vmem = pl.BlockSpec(memory_space=pltpu.VMEM)
    dma = pltpu.SemaphoreType.DMA
    flat = (NCB * CB // TR, TR)
    x_out, dual_out, weight = pl.pallas_call(
        kernel,
        out_shape=(
            jax.ShapeDtypeStruct(flat, F32),
            jax.ShapeDtypeStruct((BLOCKS, 1, TR), F32),
            jax.ShapeDtypeStruct((8, TR), F32),
        ),
        in_specs=[anywhere, vmem, vmem, vmem, vmem, vmem, anywhere, anywhere, anywhere],
        out_specs=(anywhere, vmem, vmem),
        scratch_shapes=[
            pltpu.VMEM((CH, SLOTS, TR, LANES), BF16),
            pltpu.VMEM(flat, F32),
            pltpu.VMEM(flat, F32),
            pltpu.VMEM(flat, F32),
            pltpu.VMEM((CH, NCB, LANES), BF16),
            pltpu.VMEM((NCB, TR), BF16),
            pltpu.VMEM((TR, NCB), BF16),
            pltpu.VMEM((BLOCKS, TR), F32),
            pltpu.VMEM((TR, TR), BF16),
            pltpu.VMEM((NG, GROUP, GROUP * TR), BF16),
            pltpu.VMEM((TR, LANES), F32),
            pltpu.VMEM((TR, TR), F32),
            pltpu.VMEM((TR, LANES), BF16),
            pltpu.VMEM((BLOCKS, TR), F32),
            pltpu.VMEM((TR, TR), F32),
            pltpu.VMEM((16, TR), F32),
            pltpu.VMEM((ITERS, CH, PLANE, 16, TR), BF16),
            pltpu.VMEM((ITERS, CH, PLANE, 16, TR), BF16),
            pltpu.VMEM((ITERS, CH, 16, TR), F32),
            pltpu.VMEM((ITERS, CH, ZN, 16, TR), F32),
            pltpu.VMEM((ITERS, CH, PLANE, 16, TR), BF16),
            pltpu.VMEM((ITERS, 1, TR), F32),
            pltpu.VMEM((ITERS, PLANE, 1, TR), F32),
            pltpu.VMEM((ITERS, 1, TR), F32),
            pltpu.VMEM((ITERS, ZN, 1, TR), F32),
            pltpu.VMEM((BLOCKS, 1, TR), F32),
            pltpu.VMEM((BLOCKS, 1, TR), F32),
            pltpu.VMEM((BLOCKS, TR), F32),
            dma((CH,)),
            dma((3,)),
            dma,
            dma((ITERS, CH)),
            dma((ITERS, CH)),
            dma((ITERS, CH)),
            dma((ITERS, CH)),
            dma((ITERS, CH)),
            dma((ITERS, CH)),
            dma((ITERS,)),
            dma((ITERS,)),
            dma((ITERS,)),
            dma((ITERS,)),
            dma,
            dma,
        ],
        compiler_params=pltpu.CompilerParams(
            collective_id=0, has_side_effects=True, vmem_limit_bytes=60 * 1024 * 1024
        ),
    )(
        tiles,
        col.reshape(1, SLOTS),
        counts.reshape(1, BLOCKS),
        dest.reshape(1, BLOCKS),
        bounds.reshape(BLOCKS, TR),
        dual0.reshape(BLOCKS, TR),
        primal.reshape(flat),
        cost.reshape(flat),
        upper.reshape(flat),
    )
    return pl.pallas_call(
        hand_over,
        out_shape=(
            jax.ShapeDtypeStruct((NCB * CB,), F32),
            jax.ShapeDtypeStruct((BLOCKS * TR,), F32),
            jax.ShapeDtypeStruct((1,), F32),
        ),
        in_specs=[vmem, vmem, vmem],
        out_specs=(vmem, vmem, pl.BlockSpec(memory_space=pltpu.SMEM)),
    )(x_out.reshape(-1), dual_out.reshape(-1), weight)


def solution(mesh):
    split, whole = P(GRP_DEV), P()
    return jax.shard_map(
        per_device,
        mesh=mesh,
        in_specs=(P(GRP_DEV, None, None), split, split, split, split, split, whole, whole, whole),
        out_specs=(whole, split, whole),
        check_vma=False,
    )
```

```python
import jax
import jax.numpy as jnp
from jax import lax
from jax.experimental import pallas as pl
from jax.experimental.pallas import tpu as pltpu
from jax.sharding import PartitionSpec as P

MESH = pl.DeviceIdType.MESH
GRP_DEV = ("grp", "dev")

NCB = 256
CB = 1024
TR = 128
SLOTS = 80
BLOCKS = 32
ITERS = 3
CH = 4
LANES = CB // CH
GROUP = 16
NG = SLOTS // GROUP
VSLOTS = 32
CMAT = 64
PLANE = 32
ZN = 4
STEP = 0.3

F32 = jnp.float32
BF16 = jnp.bfloat16


def iota(shape, dim):
    return lax.broadcasted_iota(jnp.int32, shape, dim)


def dot(a, b, dims=((1,), (0,)), exact=False):
    return lax.dot_general(
        a,
        b,
        (dims, ((), ())),
        precision=lax.Precision.HIGHEST if exact else None,
        preferred_element_type=F32,
    )


def kernel(
    tiles_hbm,
    col_ref,
    cnt_ref,
    dst_ref,
    bnd_ref,
    dual0_ref,
    x_hbm,
    c_hbm,
    u_hbm,
    xo_ref,
    do_ref,
    wo_ref,
    tiles,
    x,
    cost,
    upper,
    xtab,
    cmat,
    ctmat,
    omat,
    otmat,
    bd,
    prod,
    macc,
    vsel,
    vrow,
    wcol,
    wide,
    img,
    dual,
    wgt,
    snd,
    rcv,
    zsnd,
    zrcv,
    grad,
    vsnd,
    vrcv,
    vzsnd,
    vzrcv,
    dsnd,
    drcv,
    bounds,
    tile_sem,
    vec_sem,
    out_sem,
    snd_sem,
    rcv_sem,
    zsnd_sem,
    zrcv_sem,
    gs_sem,
    gr_sem,
    vs_sem,
    vr_sem,
    vzs_sem,
    vzr_sem,
    ds_sem,
    dr_sem,
):
    z = lax.axis_index("grp")
    me = lax.axis_index("dev")

    vec_copies = [
        pltpu.make_async_copy(h, v, vec_sem.at[n])
        for n, (h, v) in enumerate(((x_hbm, x), (c_hbm, cost), (u_hbm, upper)))
    ]
    vec_copies[0].start()

    def tile_copy(j):
        return pltpu.make_async_copy(
            tiles_hbm.at[:, :, pl.ds(LANES * j, LANES)], tiles.at[j], tile_sem.at[j]
        )

    tile_copy(0).start()

    along = [8 * lax.rem(me // 8 + k, 4) for k in range(4)]
    across = [2 * lax.rem(me // 2 + k, 4) for k in range(4)]
    cores = [lax.rem(me + k, 2) for k in range(2)]
    peers = [
        along[a] + across[b] + cores[c]
        for hops in (4, 3, 2, 1, 0)
        for a in range(4)
        for b in range(4)
        for c in range(2)
        if min(a, 4 - a) + min(b, 4 - b) == hops and (a, b, c) != (0, 0, 0)
    ]

    barrier = pltpu.get_barrier_semaphore()
    for peer in peers:
        pl.semaphore_signal(barrier, inc=1, device_id=(z, peer), device_id_type=MESH)
    for k in range(1, ZN):
        pl.semaphore_signal(
            barrier, inc=1, device_id=(lax.rem(z + k, ZN), me), device_id_type=MESH
        )

    def to_plane(src, dst, ssem, rsem):
        for peer in peers:
            pltpu.make_async_remote_copy(
                src_ref=src(peer),
                dst_ref=dst,
                send_sem=ssem,
                recv_sem=rsem,
                device_id=(z, peer),
                device_id_type=MESH,
            ).start()

    def to_z(src, dst, ssem, rsem, peer_z):
        pltpu.make_async_remote_copy(
            src_ref=src,
            dst_ref=dst,
            send_sem=ssem,
            recv_sem=rsem,
            device_id=(peer_z, me),
            device_id_type=MESH,
        ).start()

    def await_bytes(ref, sem):
        pltpu.make_async_copy(ref, ref, sem).wait()

    cols = jnp.broadcast_to(col_ref[...], (NCB, SLOTS))
    onehot = (cols == iota((NCB, SLOTS), 0)).astype(F32)
    onehot = jnp.concatenate([onehot, jnp.zeros((NCB, TR - SLOTS), F32)], axis=1)
    cmat[...] = onehot.astype(BF16)
    ctmat[...] = onehot.T.astype(BF16)
    counts = jnp.broadcast_to(cnt_ref[...], (TR, BLOCKS)).astype(F32)
    below = (iota((BLOCKS, BLOCKS), 1) < iota((BLOCKS, BLOCKS), 0)).astype(F32)
    upto = (iota((BLOCKS, BLOCKS), 1) <= iota((BLOCKS, BLOCKS), 0)).astype(F32)
    starts = dot(below, counts, ((1,), (1,)))
    ends = dot(upto, counts, ((1,), (1,)))
    slot = iota((BLOCKS, TR), 1).astype(F32)
    owner = jnp.where((starts <= slot) & (slot < ends), 1.0, 0.0)
    omat[...] = owner
    owner = jnp.concatenate([owner, jnp.zeros((TR - BLOCKS, TR), F32)], axis=0)
    otmat[...] = owner.T.astype(BF16)
    tile_copy(1).start()
    prod[...] = jnp.zeros_like(prod)
    macc[...] = jnp.zeros_like(macc)
    wgt[...] = jnp.ones_like(wgt)
    dual[...] = jnp.zeros_like(dual)
    dual[pl.ds(0, BLOCKS), :] = dual0_ref[...].astype(F32)
    bounds[...] = bnd_ref[...].astype(F32)

    def pieces(j, body, start):
        def row(p, carry):
            for c in range(2):
                at = pl.ds(TR * p + 2 * j + c, 16, stride=8)
                carry = body(p, c, at, carry)
            return carry

        return lax.fori_loop(0, 16, row, start, unroll=2)

    def table(j, p, c, value):
        xtab[j, pl.ds(pl.multiple_of(16 * p, 16), 16), pl.ds(TR * c, TR)] = value.astype(BF16)

    vec_copies[0].wait()
    tile_copy(2).start()
    tile_copy(3).start()
    vec_copies[1].start()
    vec_copies[2].start()
    for j in range(CH):

        def first_table(p, c, at, carry, j=j):
            table(j, p, c, x[at, :])
            return carry

        pieces(j, first_table, 0)

    def columns(it, j):
        def by_matmul(g):
            at = pl.ds(GROUP * g, GROUP)
            prod[at, :] = dot(bd[g], tiles[j, at].reshape(GROUP * TR, LANES))

        def by_vector(s):
            if j == 0:
                spot = wcol[:, s : s + 1]
                scale = jnp.broadcast_to(spot, (TR, TR))
                wide[s - CMAT] = scale
            else:
                scale = wide[s - CMAT]
            part = tiles[j, s].astype(F32)
            for c in range(2):
                lanes = pl.ds(TR * c, TR)
                some = part[:, TR * c : TR * (c + 1)] * scale
                prod[pl.ds(s, 1), lanes] = jnp.sum(some, axis=0, keepdims=True)

        left = list(range(CMAT, SLOTS))
        groups = CMAT // GROUP
        share = -(-len(left) // groups)
        for g in range(groups):
            by_matmul(g)
            for s in left[share * g : share * (g + 1)]:
                by_vector(s)
        full = prod[...]
        high = full.astype(BF16)
        low = (full - high.astype(F32)).astype(BF16)
        total = dot(cmat[...], high) + dot(cmat[...], low)
        total = total.astype(BF16)
        for c in range(2):
            snd[it, j, pl.ds(16 * c, 16)] = total[:, TR * c : TR * (c + 1)].reshape(16, 16, TR)

    def columns_out(it, j):
        to_plane(lambda i: snd.at[it, j, i], rcv.at[it, j, me], snd_sem.at[it, j], rcv_sem.at[it, j])

    def rows(j):
        picked = dot(ctmat[...], xtab[j])
        vsel[...] = picked.astype(BF16)
        vrow[...] = picked
        lane = iota((TR, TR), 1)

        def by_matmul(g, merged):
            block = tiles[j, pl.ds(GROUP * g, GROUP)].reshape(GROUP * TR, LANES)
            out = dot(block, vsel[...], ((1,), (1,)))
            for k in range(GROUP):
                merged = jnp.where(lane == GROUP * g + k, out[TR * k : TR * (k + 1)], merged)
            return merged

        def by_vector(s, merged):
            part = tiles[j, s].astype(F32) * vrow[pl.ds(s, 1), :]
            part = part[:, :TR] + part[:, TR:]
            return jnp.where(lane == s, jnp.sum(part, axis=1, keepdims=True), merged)

        merged = jnp.zeros((TR, TR), F32)
        left = list(range(SLOTS - VSLOTS, SLOTS))
        groups = (SLOTS - VSLOTS) // GROUP
        share = -(-VSLOTS // groups)
        for g in range(groups):
            merged = by_matmul(g, merged)
            for s in left[share * g : share * (g + 1)]:
                merged = by_vector(s, merged)
        macc[...] += merged

    def rows_done():
        out = dot(omat[...], macc[...], ((1,), (1,)), exact=True)
        macc[...] = jnp.zeros_like(macc)
        return out

    def plane_sum(it, j):
        rcv[it, j, me] = snd[it, j, me]
        await_bytes(rcv.at[it, j, pl.ds(0, PLANE - 1)], rcv_sem.at[it, j])
        total = rcv[it, j, 0].astype(F32)
        for i in range(1, PLANE):
            total += rcv[it, j, i].astype(F32)

        zsnd[it, j] = total
        zrcv[it, j, z] = total
        for k in range(1, ZN):
            to_z(
                zsnd.at[it, j],
                zrcv.at[it, j, z],
                zsnd_sem.at[it, j],
                zrcv_sem.at[it, j],
                lax.rem(z + k, ZN),
            )

    def spread(it, j):
        await_bytes(zrcv.at[it, j, pl.ds(0, ZN - 1)], zrcv_sem.at[it, j])
        total = zrcv[it, j, 0] + zrcv[it, j, 1] + zrcv[it, j, 2] + zrcv[it, j, 3]
        grad[it, j, me] = total.astype(BF16)
        to_plane(
            lambda i: grad.at[it, j, me], grad.at[it, j, me], gs_sem.at[it, j], gr_sem.at[it, j]
        )

    def violation_in(it, violated):
        part = violated[0:8] + violated[8:16] + violated[16:24] + violated[24:32]
        part = jnp.sum(part, axis=0, keepdims=True)
        vsnd[it] = part
        vrcv[it, me] = part

    def violation_out(it):
        to_plane(lambda i: vsnd.at[it], vrcv.at[it, me], vs_sem.at[it], vr_sem.at[it])

    def violation_plane(it):
        await_bytes(vrcv.at[it, pl.ds(0, PLANE - 1)], vr_sem.at[it])
        total = vrcv[it, 0]
        for i in range(1, PLANE):
            total += vrcv[it, i]
        vzsnd[it] = total
        vzrcv[it, z] = total
        for k in range(1, ZN):
            to_z(
                vzsnd.at[it],
                vzrcv.at[it, z],
                vzs_sem.at[it],
                vzr_sem.at[it],
                lax.rem(z + k, ZN),
            )

    def new_weight(it):
        await_bytes(vzrcv.at[it, pl.ds(0, ZN - 1)], vzr_sem.at[it])
        total = vzrcv[it, 0] + vzrcv[it, 1] + vzrcv[it, 2] + vzrcv[it, 3]
        violation = jnp.sum(total, axis=1, keepdims=True)
        change = wgt[pl.ds(8, 8), :]
        ratio = (jnp.broadcast_to(violation, (8, TR)) + 1e-6) / (change + 1e-6)
        wgt[pl.ds(0, 8), :] = jnp.sqrt(wgt[pl.ds(0, 8), :] * jnp.sqrt(ratio))

    def update(it, j, tau, moved):
        def piece(p, c, at, carry):
            old = x[at, :]
            slope = grad[it, j, 16 * c + p].astype(F32)
            new = jnp.minimum(jnp.maximum(old - tau * (cost[at, :] - slope), 0.0), upper[at, :])
            x[at, :] = new
            table(j, p, c, new)
            return carry + (new - old) * (new - old)

        return pieces(j, piece, moved)

    def iteration(it, _):
        chosen = dot(otmat[...], dual[...].astype(BF16))
        line = iota((GROUP, TR), 0)
        wcol[...] = chosen.T
        for g in range(CMAT // GROUP):
            part = chosen[GROUP * g : GROUP * (g + 1)]
            for k in range(GROUP):
                bd[g, :, pl.ds(TR * k, TR)] = jnp.where(line == k, part, 0.0).astype(BF16)
        for j in range(CH):

            @pl.when(it == 0)
            def _():
                tile_copy(j).wait()

            columns(it, j)
            if j == 0:

                @pl.when(it == 0)
                def _():
                    pl.semaphore_wait(barrier, PLANE - 1 + ZN - 1)

            columns_out(it, j)
            if j == 0:

                @pl.when(it > 0)
                def _():
                    violation_out(it - 1)

        def early_rows(j):
            @pl.when(it == 0)
            def _():
                rows(j)

        plane_sum(it, 0)

        @pl.when(it > 0)
        def _():
            violation_plane(it - 1)

        plane_sum(it, 1)
        early_rows(0)
        spread(it, 0)
        plane_sum(it, 2)
        early_rows(1)
        spread(it, 1)
        plane_sum(it, 3)
        early_rows(2)
        spread(it, 2)
        early_rows(3)

        @pl.when(it == 0)
        def _():
            img[...] = rows_done()
            vec_copies[1].wait()
            vec_copies[2].wait()

        @pl.when(it > 0)
        def _():
            new_weight(it - 1)

        weight = wgt[pl.ds(0, 1), :]
        tau = STEP / weight
        sigma = STEP * weight
        moved = jnp.zeros((16, TR), F32)
        for j in range(CH):
            await_bytes(grad.at[it, j, pl.ds(0, PLANE - 1)], gr_sem.at[it, j])
            moved = update(it, j, tau, moved)
            if j == 0:
                spread(it, CH - 1)
            rows(j)

        @pl.when(it == ITERS - 1)
        def _():
            pltpu.make_async_copy(x, xo_ref, out_sem).start()

        change = jnp.sum(jnp.sum(moved, axis=0, keepdims=True), axis=1, keepdims=True)
        wgt[pl.ds(8, 8), :] = jnp.broadcast_to(change, (8, TR))
        image = rows_done()
        violated = jnp.maximum(bounds[...] - image, 0.0)
        violation_in(it, violated * violated)
        dual[pl.ds(0, BLOCKS), :] = jnp.maximum(
            dual[pl.ds(0, BLOCKS), :] + sigma * (bounds[...] - (2.0 * image - img[...])), 0.0
        )
        img[...] = image
        return 0

    lax.fori_loop(0, ITERS, iteration, 0)

    hot = jnp.broadcast_to(dst_ref[...], (BLOCKS, BLOCKS)) == iota((BLOCKS, BLOCKS), 0)
    ordered = dot(hot.astype(F32), dual[pl.ds(0, BLOCKS), :], exact=True)
    for i in range(BLOCKS):
        dsnd[i] = ordered[i : i + 1]
    drcv[me] = dsnd[me]
    violation_out(ITERS - 1)
    to_plane(lambda i: dsnd.at[i], drcv.at[me], ds_sem, dr_sem)
    violation_plane(ITERS - 1)
    await_bytes(drcv.at[pl.ds(0, PLANE - 1)], dr_sem)
    do_ref[...] = drcv[...]
    new_weight(ITERS - 1)
    wo_ref[...] = wgt[pl.ds(0, 8), :]

    def drain(it, _):
        for j in range(CH):
            await_bytes(snd.at[it, j, pl.ds(0, PLANE - 1)], snd_sem.at[it, j])
            await_bytes(grad.at[it, j, pl.ds(0, PLANE - 1)], gs_sem.at[it, j])
            await_bytes(zrcv.at[it, j, pl.ds(0, ZN - 1)], zsnd_sem.at[it, j])

        await_bytes(vrcv.at[it, pl.ds(0, PLANE - 1)], vs_sem.at[it])
        await_bytes(vzrcv.at[it, pl.ds(0, ZN - 1)], vzs_sem.at[it])
        return 0

    lax.fori_loop(0, ITERS, drain, 0)
    await_bytes(dsnd.at[pl.ds(0, PLANE - 1)], ds_sem)
    pltpu.make_async_copy(x, xo_ref, out_sem).wait()


def hand_over(x_ref, dual_ref, weight_ref, x_out, dual_out, weight_out):
    x_out[...] = x_ref[...]
    dual_out[...] = dual_ref[...]
    weight_out[0] = weight_ref[0, 0]


def per_device(tiles, col, counts, dest, bounds, dual0, primal, cost, upper):
    anywhere = pl.BlockSpec(memory_space=pl.ANY)
    vmem = pl.BlockSpec(memory_space=pltpu.VMEM)
    dma = pltpu.SemaphoreType.DMA
    flat = (NCB * CB // TR, TR)
    x_out, dual_out, weight = pl.pallas_call(
        kernel,
        out_shape=(
            jax.ShapeDtypeStruct(flat, F32),
            jax.ShapeDtypeStruct((BLOCKS, 1, TR), F32),
            jax.ShapeDtypeStruct((8, TR), F32),
        ),
        in_specs=[anywhere, vmem, vmem, vmem, vmem, vmem, anywhere, anywhere, anywhere],
        out_specs=(anywhere, vmem, vmem),
        scratch_shapes=[
            pltpu.VMEM((CH, SLOTS, TR, LANES), BF16),
            pltpu.VMEM(flat, F32),
            pltpu.VMEM(flat, F32),
            pltpu.VMEM(flat, F32),
            pltpu.VMEM((CH, NCB, LANES), BF16),
            pltpu.VMEM((NCB, TR), BF16),
            pltpu.VMEM((TR, NCB), BF16),
            pltpu.VMEM((BLOCKS, TR), F32),
            pltpu.VMEM((TR, TR), BF16),
            pltpu.VMEM((NG, GROUP, GROUP * TR), BF16),
            pltpu.VMEM((TR, LANES), F32),
            pltpu.VMEM((TR, TR), F32),
            pltpu.VMEM((TR, LANES), BF16),
            pltpu.VMEM((TR, LANES), F32),
            pltpu.VMEM((TR, TR), F32),
            pltpu.VMEM((SLOTS - CMAT, TR, TR), F32),
            pltpu.VMEM((BLOCKS, TR), F32),
            pltpu.VMEM((TR, TR), F32),
            pltpu.VMEM((16, TR), F32),
            pltpu.VMEM((ITERS, CH, PLANE, 16, TR), BF16),
            pltpu.VMEM((ITERS, CH, PLANE, 16, TR), BF16),
            pltpu.VMEM((ITERS, CH, 16, TR), F32),
            pltpu.VMEM((ITERS, CH, ZN, 16, TR), F32),
            pltpu.VMEM((ITERS, CH, PLANE, 16, TR), BF16),
            pltpu.VMEM((ITERS, 1, TR), F32),
            pltpu.VMEM((ITERS, PLANE, 1, TR), F32),
            pltpu.VMEM((ITERS, 1, TR), F32),
            pltpu.VMEM((ITERS, ZN, 1, TR), F32),
            pltpu.VMEM((BLOCKS, 1, TR), F32),
            pltpu.VMEM((BLOCKS, 1, TR), F32),
            pltpu.VMEM((BLOCKS, TR), F32),
            dma((CH,)),
            dma((3,)),
            dma,
            dma((ITERS, CH)),
            dma((ITERS, CH)),
            dma((ITERS, CH)),
            dma((ITERS, CH)),
            dma((ITERS, CH)),
            dma((ITERS, CH)),
            dma((ITERS,)),
            dma((ITERS,)),
            dma((ITERS,)),
            dma((ITERS,)),
            dma,
            dma,
        ],
        compiler_params=pltpu.CompilerParams(
            collective_id=0, has_side_effects=True, vmem_limit_bytes=60 * 1024 * 1024
        ),
    )(
        tiles,
        col.reshape(1, SLOTS),
        counts.reshape(1, BLOCKS),
        dest.reshape(1, BLOCKS),
        bounds.reshape(BLOCKS, TR),
        dual0.reshape(BLOCKS, TR),
        primal.reshape(flat),
        cost.reshape(flat),
        upper.reshape(flat),
    )
    return pl.pallas_call(
        hand_over,
        out_shape=(
            jax.ShapeDtypeStruct((NCB * CB,), F32),
            jax.ShapeDtypeStruct((BLOCKS * TR,), F32),
            jax.ShapeDtypeStruct((1,), F32),
        ),
        in_specs=[vmem, vmem, vmem],
        out_specs=(vmem, vmem, pl.BlockSpec(memory_space=pltpu.SMEM)),
    )(x_out.reshape(-1), dual_out.reshape(-1), weight)


def solution(mesh):
    split, whole = P(GRP_DEV), P()
    return jax.shard_map(
        per_device,
        mesh=mesh,
        in_specs=(P(GRP_DEV, None, None), split, split, split, split, split, whole, whole, whole),
        out_specs=(whole, split, whole),
        check_vma=False,
    )
```

```python
import jax
import jax.numpy as jnp
from jax import lax
from jax.experimental import pallas as pl
from jax.experimental.pallas import tpu as pltpu
from jax.sharding import PartitionSpec as P

MESH = pl.DeviceIdType.MESH
GRP_DEV = ("grp", "dev")

NCB = 256
CB = 1024
TR = 128
SLOTS = 80
BLOCKS = 32
ITERS = 3
CH = 4
LANES = CB // CH
GROUP = 16
NG = SLOTS // GROUP
VSLOTS = 32
CMAT = 64
PLANE = 32
ZN = 4
STEP = 0.3

F32 = jnp.float32
BF16 = jnp.bfloat16


def iota(shape, dim):
    return lax.broadcasted_iota(jnp.int32, shape, dim)


def dot(a, b, dims=((1,), (0,)), exact=False):
    return lax.dot_general(
        a,
        b,
        (dims, ((), ())),
        precision=lax.Precision.HIGHEST if exact else None,
        preferred_element_type=F32,
    )


def kernel(
    tiles_hbm,
    col_hbm,
    cnt_hbm,
    dst_hbm,
    bnd_hbm,
    dual0_hbm,
    x_hbm,
    c_hbm,
    u_hbm,
    xo_ref,
    do_ref,
    wo_ref,
    col_ref,
    cnt_ref,
    dst_ref,
    bnd_ref,
    dual0_ref,
    tiles,
    x,
    cost,
    upper,
    xtab,
    cmat,
    ctmat,
    omat,
    otmat,
    bd,
    prod,
    macc,
    vsel,
    vrow,
    wcol,
    wide,
    img,
    dual,
    wgt,
    snd,
    rcv,
    zsnd,
    zrcv,
    grad,
    vsnd,
    vrcv,
    vzsnd,
    vzrcv,
    dsnd,
    drcv,
    bounds,
    tile_sem,
    vec_sem,
    small_sem,
    out_sem,
    snd_sem,
    rcv_sem,
    zsnd_sem,
    zrcv_sem,
    gs_sem,
    gr_sem,
    vs_sem,
    vr_sem,
    vzs_sem,
    vzr_sem,
    ds_sem,
    dr_sem,
):
    z = lax.axis_index("grp")
    me = lax.axis_index("dev")

    vec_copies = [
        pltpu.make_async_copy(h, v, vec_sem.at[n])
        for n, (h, v) in enumerate(((x_hbm, x), (c_hbm, cost), (u_hbm, upper)))
    ]

    def tile_copy(j):
        return pltpu.make_async_copy(
            tiles_hbm.at[:, :, pl.ds(LANES * j, LANES)], tiles.at[j], tile_sem.at[j]
        )

    small = (
        (col_hbm, col_ref),
        (cnt_hbm, cnt_ref),
        (dst_hbm, dst_ref),
        (bnd_hbm, bnd_ref),
        (dual0_hbm, dual0_ref),
    )
    small = [pltpu.make_async_copy(h, v, small_sem.at[n]) for n, (h, v) in enumerate(small)]
    for copy in small:
        copy.start()
    tile_copy(0).start()
    vec_copies[0].start()

    along = [8 * lax.rem(me // 8 + k, 4) for k in range(4)]
    across = [2 * lax.rem(me // 2 + k, 4) for k in range(4)]
    cores = [lax.rem(me + k, 2) for k in range(2)]
    peers = [
        along[a] + across[b] + cores[c]
        for hops in (4, 3, 2, 1, 0)
        for a in range(4)
        for b in range(4)
        for c in range(2)
        if min(a, 4 - a) + min(b, 4 - b) == hops and (a, b, c) != (0, 0, 0)
    ]

    barrier = pltpu.get_barrier_semaphore()
    for peer in peers:
        pl.semaphore_signal(barrier, inc=1, device_id=(z, peer), device_id_type=MESH)
    for k in (2, 1, 3):
        pl.semaphore_signal(
            barrier, inc=1, device_id=(lax.rem(z + k, ZN), me), device_id_type=MESH
        )

    def to_plane(src, dst, ssem, rsem):
        for peer in peers:
            pltpu.make_async_remote_copy(
                src_ref=src(peer),
                dst_ref=dst,
                send_sem=ssem,
                recv_sem=rsem,
                device_id=(z, peer),
                device_id_type=MESH,
            ).start()

    def to_z(src, dst, ssem, rsem, peer_z):
        pltpu.make_async_remote_copy(
            src_ref=src,
            dst_ref=dst,
            send_sem=ssem,
            recv_sem=rsem,
            device_id=(peer_z, me),
            device_id_type=MESH,
        ).start()

    def await_bytes(ref, sem):
        pltpu.make_async_copy(ref, ref, sem).wait()

    for copy in small:
        copy.wait()
    cols = jnp.broadcast_to(col_ref[...], (NCB, SLOTS))
    onehot = (cols == iota((NCB, SLOTS), 0)).astype(F32)
    onehot = jnp.concatenate([onehot, jnp.zeros((NCB, TR - SLOTS), F32)], axis=1)
    cmat[...] = onehot.astype(BF16)
    ctmat[...] = onehot.T.astype(BF16)
    counts = jnp.broadcast_to(cnt_ref[...], (TR, BLOCKS)).astype(F32)
    below = (iota((BLOCKS, BLOCKS), 1) < iota((BLOCKS, BLOCKS), 0)).astype(F32)
    upto = (iota((BLOCKS, BLOCKS), 1) <= iota((BLOCKS, BLOCKS), 0)).astype(F32)
    starts = dot(below, counts, ((1,), (1,)))
    ends = dot(upto, counts, ((1,), (1,)))
    slot = iota((BLOCKS, TR), 1).astype(F32)
    owner = jnp.where((starts <= slot) & (slot < ends), 1.0, 0.0)
    omat[...] = owner
    owner = jnp.concatenate([owner, jnp.zeros((TR - BLOCKS, TR), F32)], axis=0)
    otmat[...] = owner.T.astype(BF16)
    prod[...] = jnp.zeros_like(prod)
    macc[...] = jnp.zeros_like(macc)
    wgt[...] = jnp.ones_like(wgt)
    dual[...] = jnp.zeros_like(dual)
    dual[pl.ds(0, BLOCKS), :] = dual0_ref[...].astype(F32)
    bounds[...] = bnd_ref[...].astype(F32)

    def pieces(j, body, start):
        def row(p, carry):
            for c in range(2):
                at = pl.ds(TR * p + 2 * j + c, 16, stride=8)
                carry = body(p, c, at, carry)
            return carry

        return lax.fori_loop(0, 16, row, start, unroll=4)

    def table(j, p, c, value):
        xtab[j, pl.ds(pl.multiple_of(16 * p, 16), 16), pl.ds(TR * c, TR)] = value.astype(BF16)

    def first_table(j):
        def fill(p, c, at, carry):
            table(j, p, c, x[at, :])
            return carry

        pieces(j, fill, 0)

    def columns(it, j, first):
        def by_matmul(g):
            at = pl.ds(GROUP * g, GROUP)
            prod[at, :] = dot(bd[g], tiles[j, at].reshape(GROUP * TR, LANES))

        def by_vector(s):
            if first:
                spot = wcol[:, s : s + 1]
                scale = jnp.broadcast_to(spot, (TR, TR))
                wide[s - CMAT] = scale
            else:
                scale = wide[s - CMAT]
            part = tiles[j, s].astype(F32)
            for c in range(2):
                lanes = pl.ds(TR * c, TR)
                some = part[:, TR * c : TR * (c + 1)] * scale
                prod[pl.ds(s, 1), lanes] = jnp.sum(some, axis=0, keepdims=True)

        left = list(range(CMAT, SLOTS))
        groups = CMAT // GROUP
        share = -(-len(left) // groups)
        for g in range(groups):
            by_matmul(g)
            for s in left[share * g : share * (g + 1)]:
                by_vector(s)
        full = prod[...]
        high = full.astype(BF16)
        low = (full - high.astype(F32)).astype(BF16)
        total = dot(cmat[...], high) + dot(cmat[...], low)
        total = total.astype(BF16)
        for c in range(2):
            snd[it, j, pl.ds(16 * c, 16)] = total[:, TR * c : TR * (c + 1)].reshape(16, 16, TR)

    def columns_out(it, j):
        to_plane(lambda i: snd.at[it, j, i], rcv.at[it, j, me], snd_sem.at[it, j], rcv_sem.at[it, j])

    def rows(j):
        picked = dot(ctmat[...], xtab[j])
        vsel[...] = picked.astype(BF16)
        vrow[...] = picked
        lane = iota((TR, TR), 1)

        def by_matmul(g, merged):
            block = tiles[j, pl.ds(GROUP * g, GROUP)].reshape(GROUP * TR, LANES)
            out = dot(block, vsel[...], ((1,), (1,)))
            for k in range(GROUP):
                merged = jnp.where(lane == GROUP * g + k, out[TR * k : TR * (k + 1)], merged)
            return merged

        def by_vector(s, merged):
            part = tiles[j, s].astype(F32) * vrow[pl.ds(s, 1), :]
            part = part[:, :TR] + part[:, TR:]
            return jnp.where(lane == s, jnp.sum(part, axis=1, keepdims=True), merged)

        merged = jnp.zeros((TR, TR), F32)
        left = list(range(SLOTS - VSLOTS, SLOTS))
        groups = (SLOTS - VSLOTS) // GROUP
        share = -(-VSLOTS // groups)
        for g in range(groups):
            merged = by_matmul(g, merged)
            for s in left[share * g : share * (g + 1)]:
                merged = by_vector(s, merged)
        macc[...] += merged

    def rows_done():
        out = dot(omat[...], macc[...], ((1,), (1,)), exact=True)
        macc[...] = jnp.zeros_like(macc)
        return out

    def plane_sum(it, j):
        rcv[it, j, me] = snd[it, j, me]
        await_bytes(rcv.at[it, j, pl.ds(0, PLANE - 1)], rcv_sem.at[it, j])
        total = rcv[it, j, 0].astype(F32)
        for i in range(1, PLANE):
            total += rcv[it, j, i].astype(F32)

        zsnd[it, j] = total
        zrcv[it, j, z] = total
        for k in (2, 1, 3):
            to_z(
                zsnd.at[it, j],
                zrcv.at[it, j, z],
                zsnd_sem.at[it, j],
                zrcv_sem.at[it, j],
                lax.rem(z + k, ZN),
            )

    def spread(it, j):
        await_bytes(zrcv.at[it, j, pl.ds(0, ZN - 1)], zrcv_sem.at[it, j])
        total = zrcv[it, j, 0] + zrcv[it, j, 1] + zrcv[it, j, 2] + zrcv[it, j, 3]
        grad[it, j, me] = total.astype(BF16)
        to_plane(
            lambda i: grad.at[it, j, me], grad.at[it, j, me], gs_sem.at[it, j], gr_sem.at[it, j]
        )

    def violation_in(it, violated):
        part = violated[0:8] + violated[8:16] + violated[16:24] + violated[24:32]
        part = jnp.sum(part, axis=0, keepdims=True)
        vsnd[it] = part
        vrcv[it, me] = part

    def violation_out(it):
        to_plane(lambda i: vsnd.at[it], vrcv.at[it, me], vs_sem.at[it], vr_sem.at[it])

    def violation_plane(it):
        await_bytes(vrcv.at[it, pl.ds(0, PLANE - 1)], vr_sem.at[it])
        total = vrcv[it, 0]
        for i in range(1, PLANE):
            total += vrcv[it, i]
        vzsnd[it] = total
        vzrcv[it, z] = total
        for k in (2, 1, 3):
            to_z(
                vzsnd.at[it],
                vzrcv.at[it, z],
                vzs_sem.at[it],
                vzr_sem.at[it],
                lax.rem(z + k, ZN),
            )

    def new_weight(it):
        await_bytes(vzrcv.at[it, pl.ds(0, ZN - 1)], vzr_sem.at[it])
        total = vzrcv[it, 0] + vzrcv[it, 1] + vzrcv[it, 2] + vzrcv[it, 3]
        violation = jnp.sum(total, axis=1, keepdims=True)
        change = wgt[pl.ds(8, 8), :]
        ratio = (jnp.broadcast_to(violation, (8, TR)) + 1e-6) / (change + 1e-6)
        wgt[pl.ds(0, 8), :] = jnp.sqrt(wgt[pl.ds(0, 8), :] * jnp.sqrt(ratio))

    def update(it, j, tau, moved):
        def piece(p, c, at, carry):
            old = x[at, :]
            slope = grad[it, j, 16 * c + p].astype(F32)
            new = jnp.minimum(jnp.maximum(old - tau * (cost[at, :] - slope), 0.0), upper[at, :])
            x[at, :] = new
            table(j, p, c, new)
            return carry + (new - old) * (new - old)

        return pieces(j, piece, moved)

    def iteration(it, _):
        chosen = dot(otmat[...], dual[...].astype(BF16))
        line = iota((GROUP, TR), 0)
        wcol[...] = chosen.T
        for g in range(CMAT // GROUP):
            part = chosen[GROUP * g : GROUP * (g + 1)]
            for k in range(GROUP):
                bd[g, :, pl.ds(TR * k, TR)] = jnp.where(line == k, part, 0.0).astype(BF16)
        @pl.when(it == 0)
        def _():
            tile_copy(1).start()
            tile_copy(0).wait()
            for j in range(2, CH):
                tile_copy(j).start()
            vec_copies[1].start()
            vec_copies[2].start()

        columns(it, 0, True)

        @pl.when(it == 0)
        def _():
            pl.semaphore_wait(barrier, PLANE - 1 + ZN - 1)

        columns_out(it, 0)

        @pl.when(it == 0)
        def _():
            vec_copies[0].wait()
            first_table(0)

        def later(j, _):
            @pl.when(it == 0)
            def _():
                first_table(j)
                tile_copy(j).wait()

            columns(it, j, False)
            columns_out(it, j)
            return 0

        lax.fori_loop(1, CH, later, 0)

        def early_rows(j):
            @pl.when(it == 0)
            def _():
                rows(j)

        @pl.when(it > 0)
        def _():
            violation_out(it - 1)

        plane_sum(it, 0)
        early_rows(0)
        plane_sum(it, 1)

        @pl.when(it == 0)
        def _():
            spread(it, 0)
            plane_sum(it, 2)
            rows(1)

        @pl.when(it > 0)
        def _():
            plane_sum(it, 2)
            spread(it, 0)
            plane_sum(it, 3)

        spread(it, 1)

        @pl.when(it == 0)
        def _():
            plane_sum(it, 3)
            rows(2)

        @pl.when(it > 0)
        def _():
            violation_plane(it - 1)

        spread(it, 2)
        early_rows(3)
        spread(it, 3)

        @pl.when(it == 0)
        def _():
            img[...] = rows_done()
            vec_copies[1].wait()
            vec_copies[2].wait()

        @pl.when(it > 0)
        def _():
            new_weight(it - 1)

        weight = wgt[pl.ds(0, 1), :]
        tau = STEP / weight
        sigma = STEP * weight
        moved = jnp.zeros((16, TR), F32)
        def step(j, moved):
            await_bytes(grad.at[it, j, pl.ds(0, PLANE - 1)], gr_sem.at[it, j])
            moved = update(it, j, tau, moved)
            rows(j)
            return moved

        moved = lax.fori_loop(0, CH, step, moved)

        @pl.when(it == ITERS - 1)
        def _():
            pltpu.make_async_copy(x, xo_ref, out_sem).start()

        change = jnp.sum(jnp.sum(moved, axis=0, keepdims=True), axis=1, keepdims=True)
        wgt[pl.ds(8, 8), :] = jnp.broadcast_to(change, (8, TR))
        image = rows_done()
        violated = jnp.maximum(bounds[...] - image, 0.0)
        violation_in(it, violated * violated)
        dual[pl.ds(0, BLOCKS), :] = jnp.maximum(
            dual[pl.ds(0, BLOCKS), :] + sigma * (bounds[...] - (2.0 * image - img[...])), 0.0
        )
        img[...] = image
        return 0

    lax.fori_loop(0, ITERS, iteration, 0)

    hot = jnp.broadcast_to(dst_ref[...], (BLOCKS, BLOCKS)) == iota((BLOCKS, BLOCKS), 0)
    ordered = dot(hot.astype(F32), dual[pl.ds(0, BLOCKS), :], exact=True)
    for i in range(BLOCKS):
        dsnd[i] = ordered[i : i + 1]
    drcv[me] = dsnd[me]
    violation_out(ITERS - 1)
    to_plane(lambda i: dsnd.at[i], drcv.at[me], ds_sem, dr_sem)
    violation_plane(ITERS - 1)
    await_bytes(drcv.at[pl.ds(0, PLANE - 1)], dr_sem)
    do_ref[...] = drcv[...]
    new_weight(ITERS - 1)
    wo_ref[...] = wgt[pl.ds(0, 8), :]

    def drain(it, _):
        for j in range(CH):
            await_bytes(snd.at[it, j, pl.ds(0, PLANE - 1)], snd_sem.at[it, j])
            await_bytes(grad.at[it, j, pl.ds(0, PLANE - 1)], gs_sem.at[it, j])
            await_bytes(zrcv.at[it, j, pl.ds(0, ZN - 1)], zsnd_sem.at[it, j])

        await_bytes(vrcv.at[it, pl.ds(0, PLANE - 1)], vs_sem.at[it])
        await_bytes(vzrcv.at[it, pl.ds(0, ZN - 1)], vzs_sem.at[it])
        return 0

    lax.fori_loop(0, ITERS, drain, 0)
    await_bytes(dsnd.at[pl.ds(0, PLANE - 1)], ds_sem)
    pltpu.make_async_copy(x, xo_ref, out_sem).wait()


def hand_over(x_in, dual_in, weight_in, x_out, dual_out, weight_out, x, dual, weight, one, sem):
    part = NCB * CB // 4
    ins, outs = [], []
    for n in range(4):
        at = pl.ds(part * n, part)
        ins.append(pltpu.make_async_copy(x_in.at[at], x.at[at], sem.at[n]))
        outs.append(pltpu.make_async_copy(x.at[at], x_out.at[at], sem.at[6 + n]))
    ins.append(pltpu.make_async_copy(dual_in, dual, sem.at[4]))
    outs.append(pltpu.make_async_copy(dual, dual_out, sem.at[10]))
    last_in = pltpu.make_async_copy(weight_in, weight, sem.at[5])
    last_out = pltpu.make_async_copy(one, weight_out, sem.at[11])
    last_in.start()
    for copy in ins:
        copy.start()
    last_in.wait()
    one[0] = weight[0, 0]
    last_out.start()
    for copy, after in zip(ins, outs):
        copy.wait()
        after.start()
    for copy in outs:
        copy.wait()
    last_out.wait()


def per_device(tiles, col, counts, dest, bounds, dual0, primal, cost, upper):
    vmem = pl.BlockSpec(memory_space=pltpu.VMEM)
    anywhere = pl.BlockSpec(memory_space=pl.ANY)
    dma = pltpu.SemaphoreType.DMA
    flat = (NCB * CB // TR, TR)
    x_out, dual_out, weight = pl.pallas_call(
        kernel,
        out_shape=(
            jax.ShapeDtypeStruct(flat, F32),
            jax.ShapeDtypeStruct((BLOCKS, 1, TR), F32),
            jax.ShapeDtypeStruct((8, TR), F32),
        ),
        in_specs=[anywhere] * 9,
        out_specs=(anywhere, vmem, vmem),
        scratch_shapes=[
            pltpu.VMEM((1, SLOTS), jnp.int32),
            pltpu.VMEM((1, BLOCKS), jnp.int32),
            pltpu.VMEM((1, BLOCKS), jnp.int32),
            pltpu.VMEM((BLOCKS, TR), BF16),
            pltpu.VMEM((BLOCKS, TR), BF16),
            pltpu.VMEM((CH, SLOTS, TR, LANES), BF16),
            pltpu.VMEM(flat, F32),
            pltpu.VMEM(flat, F32),
            pltpu.VMEM(flat, F32),
            pltpu.VMEM((CH, NCB, LANES), BF16),
            pltpu.VMEM((NCB, TR), BF16),
            pltpu.VMEM((TR, NCB), BF16),
            pltpu.VMEM((BLOCKS, TR), F32),
            pltpu.VMEM((TR, TR), BF16),
            pltpu.VMEM((NG, GROUP, GROUP * TR), BF16),
            pltpu.VMEM((TR, LANES), F32),
            pltpu.VMEM((TR, TR), F32),
            pltpu.VMEM((TR, LANES), BF16),
            pltpu.VMEM((TR, LANES), F32),
            pltpu.VMEM((TR, TR), F32),
            pltpu.VMEM((SLOTS - CMAT, TR, TR), F32),
            pltpu.VMEM((BLOCKS, TR), F32),
            pltpu.VMEM((TR, TR), F32),
            pltpu.VMEM((16, TR), F32),
            pltpu.VMEM((ITERS, CH, PLANE, 16, TR), BF16),
            pltpu.VMEM((ITERS, CH, PLANE, 16, TR), BF16),
            pltpu.VMEM((ITERS, CH, 16, TR), F32),
            pltpu.VMEM((ITERS, CH, ZN, 16, TR), F32),
            pltpu.VMEM((ITERS, CH, PLANE, 16, TR), BF16),
            pltpu.VMEM((ITERS, 1, TR), F32),
            pltpu.VMEM((ITERS, PLANE, 1, TR), F32),
            pltpu.VMEM((ITERS, 1, TR), F32),
            pltpu.VMEM((ITERS, ZN, 1, TR), F32),
            pltpu.VMEM((BLOCKS, 1, TR), F32),
            pltpu.VMEM((BLOCKS, 1, TR), F32),
            pltpu.VMEM((BLOCKS, TR), F32),
            dma((CH,)),
            dma((3,)),
            dma((5,)),
            dma,
            dma((ITERS, CH)),
            dma((ITERS, CH)),
            dma((ITERS, CH)),
            dma((ITERS, CH)),
            dma((ITERS, CH)),
            dma((ITERS, CH)),
            dma((ITERS,)),
            dma((ITERS,)),
            dma((ITERS,)),
            dma((ITERS,)),
            dma,
            dma,
        ],
        compiler_params=pltpu.CompilerParams(
            collective_id=0, has_side_effects=True, vmem_limit_bytes=60 * 1024 * 1024
        ),
    )(
        tiles,
        col.reshape(1, SLOTS),
        counts.reshape(1, BLOCKS),
        dest.reshape(1, BLOCKS),
        bounds.reshape(BLOCKS, TR),
        dual0.reshape(BLOCKS, TR),
        primal.reshape(flat),
        cost.reshape(flat),
        upper.reshape(flat),
    )
    return pl.pallas_call(
        hand_over,
        out_shape=(
            jax.ShapeDtypeStruct((NCB * CB,), F32),
            jax.ShapeDtypeStruct((BLOCKS * TR,), F32),
            jax.ShapeDtypeStruct((1,), F32),
        ),
        in_specs=[anywhere] * 3,
        out_specs=(anywhere, anywhere, anywhere),
        scratch_shapes=[
            pltpu.VMEM((NCB * CB,), F32),
            pltpu.VMEM((BLOCKS * TR,), F32),
            pltpu.VMEM((8, TR), F32),
            pltpu.SMEM((1,), F32),
            dma((12,)),
        ],
    )(x_out.reshape(-1), dual_out.reshape(-1), weight)


def solution(mesh):
    split, whole = P(GRP_DEV), P()
    return jax.shard_map(
        per_device,
        mesh=mesh,
        in_specs=(P(GRP_DEV, None, None), split, split, split, split, split, whole, whole, whole),
        out_specs=(whole, split, whole),
        check_vma=False,
    )
```

```python
import jax
import jax.numpy as jnp
from jax import lax
from jax.experimental import pallas as pl
from jax.experimental.pallas import tpu as pltpu
from jax.sharding import PartitionSpec as P

MESH = pl.DeviceIdType.MESH
GRP_DEV = ("grp", "dev")

NCB = 256
CB = 1024
TR = 128
SLOTS = 80
BLOCKS = 32
ITERS = 3
CH = 4
LANES = CB // CH
GROUP = 16
NG = SLOTS // GROUP
VSLOTS = 40
RGROUP = 8
CMAT = 64
PLANE = 32
ZN = 4
STEP = 0.3

F32 = jnp.float32
BF16 = jnp.bfloat16


def iota(shape, dim):
    return lax.broadcasted_iota(jnp.int32, shape, dim)


def dot(a, b, dims=((1,), (0,)), exact=False):
    return lax.dot_general(
        a,
        b,
        (dims, ((), ())),
        precision=lax.Precision.HIGHEST if exact else None,
        preferred_element_type=F32,
    )


def kernel(
    tiles_hbm,
    col_hbm,
    cnt_hbm,
    dst_hbm,
    bnd_hbm,
    dual0_hbm,
    x_hbm,
    c_hbm,
    u_hbm,
    xo_ref,
    do_ref,
    wo_ref,
    col_ref,
    cnt_ref,
    dst_ref,
    bnd_ref,
    dual0_ref,
    tiles,
    x,
    cost,
    upper,
    xtab,
    cmat,
    ctmat,
    omat,
    otmat,
    bd,
    prod,
    macc,
    vsel,
    vrow,
    wcol,
    wide,
    img,
    dual,
    wgt,
    snd,
    rcv,
    zsnd,
    zrcv,
    grad,
    vsnd,
    vrcv,
    vzsnd,
    vzrcv,
    dsnd,
    drcv,
    bounds,
    tile_sem,
    vec_sem,
    small_sem,
    out_sem,
    last_sem,
    snd_sem,
    rcv_sem,
    zsnd_sem,
    zrcv_sem,
    gs_sem,
    gr_sem,
    vs_sem,
    vr_sem,
    vzs_sem,
    vzr_sem,
    ds_sem,
    dr_sem,
):
    z = lax.axis_index("grp")
    me = lax.axis_index("dev")

    vec_copies = [
        pltpu.make_async_copy(h, v, vec_sem.at[n])
        for n, (h, v) in enumerate(((x_hbm, x), (c_hbm, cost), (u_hbm, upper)))
    ]

    def tile_copy(j):
        return pltpu.make_async_copy(
            tiles_hbm.at[:, :, pl.ds(LANES * j, LANES)], tiles.at[j], tile_sem.at[j]
        )

    small = (
        (col_hbm, col_ref),
        (cnt_hbm, cnt_ref),
        (dst_hbm, dst_ref),
        (bnd_hbm, bnd_ref),
        (dual0_hbm, dual0_ref),
    )
    small = [pltpu.make_async_copy(h, v, small_sem.at[n]) for n, (h, v) in enumerate(small)]
    for copy in small:
        copy.start()
    tile_copy(0).start()
    vec_copies[0].start()

    along = [8 * lax.rem(me // 8 + k, 4) for k in range(4)]
    across = [2 * lax.rem(me // 2 + k, 4) for k in range(4)]
    cores = [lax.rem(me + k, 2) for k in range(2)]
    peers = [
        along[a] + across[b] + cores[c]
        for hops in (4, 3, 2, 1, 0)
        for a in range(4)
        for b in range(4)
        for c in range(2)
        if min(a, 4 - a) + min(b, 4 - b) == hops and (a, b, c) != (0, 0, 0)
    ]

    barrier = pltpu.get_barrier_semaphore()
    for peer in peers:
        pl.semaphore_signal(barrier, inc=1, device_id=(z, peer), device_id_type=MESH)
    for k in (2, 1, 3):
        pl.semaphore_signal(
            barrier, inc=1, device_id=(lax.rem(z + k, ZN), me), device_id_type=MESH
        )

    def to_plane(src, dst, ssem, rsem):
        for peer in peers:
            pltpu.make_async_remote_copy(
                src_ref=src(peer),
                dst_ref=dst,
                send_sem=ssem,
                recv_sem=rsem,
                device_id=(z, peer),
                device_id_type=MESH,
            ).start()

    def to_z(src, dst, ssem, rsem, peer_z):
        pltpu.make_async_remote_copy(
            src_ref=src,
            dst_ref=dst,
            send_sem=ssem,
            recv_sem=rsem,
            device_id=(peer_z, me),
            device_id_type=MESH,
        ).start()

    def await_bytes(ref, sem):
        pltpu.make_async_copy(ref, ref, sem).wait()

    for copy in small:
        copy.wait()
    cols = jnp.broadcast_to(col_ref[...], (NCB, SLOTS))
    onehot = (cols == iota((NCB, SLOTS), 0)).astype(F32)
    onehot = jnp.concatenate([onehot, jnp.zeros((NCB, TR - SLOTS), F32)], axis=1)
    cmat[...] = onehot.astype(BF16)
    ctmat[...] = onehot.T.astype(BF16)
    counts = jnp.broadcast_to(cnt_ref[...], (TR, BLOCKS)).astype(F32)
    below = (iota((BLOCKS, BLOCKS), 1) < iota((BLOCKS, BLOCKS), 0)).astype(F32)
    upto = (iota((BLOCKS, BLOCKS), 1) <= iota((BLOCKS, BLOCKS), 0)).astype(F32)
    starts = dot(below, counts, ((1,), (1,)))
    ends = dot(upto, counts, ((1,), (1,)))
    slot = iota((BLOCKS, TR), 1).astype(F32)
    owner = jnp.where((starts <= slot) & (slot < ends), 1.0, 0.0)
    omat[:, :TR] = owner.astype(BF16)
    omat[:, TR:] = owner.astype(BF16)
    owner = jnp.concatenate([owner, jnp.zeros((TR - BLOCKS, TR), F32)], axis=0)
    otmat[...] = owner.T.astype(BF16)
    prod[...] = jnp.zeros_like(prod)
    macc[...] = jnp.zeros_like(macc)
    wgt[...] = jnp.ones_like(wgt)
    dual[...] = jnp.zeros_like(dual)
    dual[pl.ds(0, BLOCKS), :] = dual0_ref[...].astype(F32)
    bounds[...] = bnd_ref[...].astype(F32)

    def pieces(j, body, start):
        def row(p, carry):
            for c in range(2):
                at = pl.ds(TR * p + 2 * j + c, 16, stride=8)
                carry = body(p, c, at, carry)
            return carry

        return lax.fori_loop(0, 16, row, start, unroll=4)

    def table(j, p, c, value):
        xtab[j, pl.ds(pl.multiple_of(16 * p, 16), 16), pl.ds(TR * c, TR)] = value.astype(BF16)

    def first_table(j):
        def fill(p, c, at, carry):
            table(j, p, c, x[at, :])
            return carry

        pieces(j, fill, 0)

    def columns(it, j, first):
        def by_matmul(g):
            at = pl.ds(GROUP * g, GROUP)
            prod[at, :] = dot(bd[g], tiles[j, at].reshape(GROUP * TR, LANES))

        def by_vector(s):
            if first:
                spot = wcol[:, s : s + 1]
                scale = jnp.broadcast_to(spot, (TR, TR))
                wide[s - CMAT] = scale
            else:
                scale = wide[s - CMAT]
            part = tiles[j, s].astype(F32)
            for c in range(2):
                lanes = pl.ds(TR * c, TR)
                some = part[:, TR * c : TR * (c + 1)] * scale
                prod[pl.ds(s, 1), lanes] = jnp.sum(some, axis=0, keepdims=True)

        left = list(range(CMAT, SLOTS))
        groups = CMAT // GROUP
        share = -(-len(left) // groups)
        for g in range(groups):
            by_matmul(g)
            for s in left[share * g : share * (g + 1)]:
                by_vector(s)
        full = prod[...]
        high = full.astype(BF16)
        low = (full - high.astype(F32)).astype(BF16)
        total = dot(cmat[...], high) + dot(cmat[...], low)
        total = total.astype(BF16)
        for c in range(2):
            snd[it, j, pl.ds(16 * c, 16)] = total[:, TR * c : TR * (c + 1)].reshape(16, 16, TR)

    def columns_out(it, j):
        to_plane(lambda i: snd.at[it, j, i], rcv.at[it, j, me], snd_sem.at[it, j], rcv_sem.at[it, j])

    def rows(j):
        picked = dot(ctmat[...], xtab[j])
        vsel[...] = picked.astype(BF16)
        vrow[...] = picked
        lane = iota((TR, TR), 1)

        def by_matmul(g, merged):
            block = tiles[j, pl.ds(RGROUP * g, RGROUP)].reshape(RGROUP * TR, LANES)
            out = dot(block, vsel[...], ((1,), (1,)))
            for k in range(RGROUP):
                merged = jnp.where(lane == RGROUP * g + k, out[TR * k : TR * (k + 1)], merged)
            return merged

        def by_vector(s, merged):
            part = tiles[j, s].astype(F32) * vrow[pl.ds(s, 1), :]
            part = part[:, :TR] + part[:, TR:]
            return jnp.where(lane == s, jnp.sum(part, axis=1, keepdims=True), merged)

        merged = jnp.zeros((TR, TR), F32)
        left = list(range(SLOTS - VSLOTS, SLOTS))
        groups = (SLOTS - VSLOTS) // RGROUP
        share = -(-VSLOTS // groups)
        for g in range(groups):
            merged = by_matmul(g, merged)
            for s in left[share * g : share * (g + 1)]:
                merged = by_vector(s, merged)
        macc[...] += merged

    def rows_done():
        full = macc[...]
        high = full.astype(BF16)
        low = (full - high.astype(F32)).astype(BF16)
        out = dot(omat[...], jnp.concatenate([high, low], axis=1), ((1,), (1,)))
        macc[...] = jnp.zeros_like(macc)
        return out

    def plane_sum(it, j):
        rcv[it, j, me] = snd[it, j, me]
        await_bytes(rcv.at[it, j, pl.ds(0, PLANE - 1)], rcv_sem.at[it, j])
        total = rcv[it, j, 0].astype(F32)
        for i in range(1, PLANE):
            total += rcv[it, j, i].astype(F32)

        zsnd[it, j] = total
        zrcv[it, j, z] = total
        for k in (2, 1, 3):
            to_z(
                zsnd.at[it, j],
                zrcv.at[it, j, z],
                zsnd_sem.at[it, j],
                zrcv_sem.at[it, j],
                lax.rem(z + k, ZN),
            )

    def spread(it, j):
        await_bytes(zrcv.at[it, j, pl.ds(0, ZN - 1)], zrcv_sem.at[it, j])
        total = zrcv[it, j, 0] + zrcv[it, j, 1] + zrcv[it, j, 2] + zrcv[it, j, 3]
        grad[it, j, me] = total.astype(BF16)
        to_plane(
            lambda i: grad.at[it, j, me], grad.at[it, j, me], gs_sem.at[it, j], gr_sem.at[it, j]
        )

    def violation_in(it, violated):
        part = violated[0:8] + violated[8:16] + violated[16:24] + violated[24:32]
        part = jnp.sum(part, axis=0, keepdims=True)
        vsnd[it] = part
        vrcv[it, me] = part

    def violation_out(it):
        to_plane(lambda i: vsnd.at[it], vrcv.at[it, me], vs_sem.at[it], vr_sem.at[it])

    def violation_plane(it):
        await_bytes(vrcv.at[it, pl.ds(0, PLANE - 1)], vr_sem.at[it])
        total = vrcv[it, 0]
        for i in range(1, PLANE):
            total += vrcv[it, i]
        vzsnd[it] = total
        vzrcv[it, z] = total
        for k in (2, 1, 3):
            to_z(
                vzsnd.at[it],
                vzrcv.at[it, z],
                vzs_sem.at[it],
                vzr_sem.at[it],
                lax.rem(z + k, ZN),
            )

    def new_weight(it):
        await_bytes(vzrcv.at[it, pl.ds(0, ZN - 1)], vzr_sem.at[it])
        total = vzrcv[it, 0] + vzrcv[it, 1] + vzrcv[it, 2] + vzrcv[it, 3]
        violation = jnp.sum(total, axis=1, keepdims=True)
        change = wgt[pl.ds(8, 8), :]
        ratio = (jnp.broadcast_to(violation, (8, TR)) + 1e-6) / (change + 1e-6)
        wgt[pl.ds(0, 8), :] = jnp.sqrt(wgt[pl.ds(0, 8), :] * jnp.sqrt(ratio))

    def update(it, j, tau, moved):
        def piece(p, c, at, carry):
            old = x[at, :]
            slope = grad[it, j, 16 * c + p].astype(F32)
            new = jnp.minimum(jnp.maximum(old - tau * (cost[at, :] - slope), 0.0), upper[at, :])
            x[at, :] = new
            table(j, p, c, new)
            return carry + (new - old) * (new - old)

        return pieces(j, piece, moved)

    def iteration(it, _):
        chosen = dot(otmat[...], dual[...].astype(BF16))
        line = iota((GROUP, TR), 0)
        wcol[...] = chosen.T
        for g in range(CMAT // GROUP):
            part = chosen[GROUP * g : GROUP * (g + 1)]
            for k in range(GROUP):
                bd[g, :, pl.ds(TR * k, TR)] = jnp.where(line == k, part, 0.0).astype(BF16)
        @pl.when(it == 0)
        def _():
            tile_copy(1).start()
            tile_copy(0).wait()
            for j in range(2, CH):
                tile_copy(j).start()
            vec_copies[1].start()
            vec_copies[2].start()

        columns(it, 0, True)

        @pl.when(it == 0)
        def _():
            pl.semaphore_wait(barrier, PLANE - 1 + ZN - 1)

        columns_out(it, 0)

        @pl.when(it == 0)
        def _():
            vec_copies[0].wait()
            first_table(0)

        def later(j, _):
            @pl.when(it == 0)
            def _():
                first_table(j)
                tile_copy(j).wait()

            columns(it, j, False)
            columns_out(it, j)
            return 0

        lax.fori_loop(1, CH, later, 0)

        def early_rows(j):
            @pl.when(it == 0)
            def _():
                rows(j)

        @pl.when(it > 0)
        def _():
            violation_out(it - 1)

        plane_sum(it, 0)
        early_rows(0)
        plane_sum(it, 1)

        @pl.when(it == 0)
        def _():
            spread(it, 0)
            plane_sum(it, 2)
            rows(1)

        @pl.when(it > 0)
        def _():
            plane_sum(it, 2)
            spread(it, 0)
            plane_sum(it, 3)

        spread(it, 1)

        @pl.when(it == 0)
        def _():
            plane_sum(it, 3)
            rows(2)

        @pl.when(it > 0)
        def _():
            violation_plane(it - 1)

        spread(it, 2)
        early_rows(3)
        spread(it, 3)

        @pl.when(it == 0)
        def _():
            img[...] = rows_done()
            vec_copies[1].wait()
            vec_copies[2].wait()

        @pl.when(it > 0)
        def _():
            new_weight(it - 1)

        weight = wgt[pl.ds(0, 1), :]
        tau = STEP / weight
        sigma = STEP * weight
        moved = jnp.zeros((16, TR), F32)
        def step(j, moved):
            await_bytes(grad.at[it, j, pl.ds(0, PLANE - 1)], gr_sem.at[it, j])
            moved = update(it, j, tau, moved)
            rows(j)
            return moved

        moved = lax.fori_loop(0, CH, step, moved)

        @pl.when(it == ITERS - 1)
        def _():
            pltpu.make_async_copy(x, xo_ref, out_sem).start()

        change = jnp.sum(jnp.sum(moved, axis=0, keepdims=True), axis=1, keepdims=True)
        wgt[pl.ds(8, 8), :] = jnp.broadcast_to(change, (8, TR))
        image = rows_done()
        violated = jnp.maximum(bounds[...] - image, 0.0)
        violation_in(it, violated * violated)
        dual[pl.ds(0, BLOCKS), :] = jnp.maximum(
            dual[pl.ds(0, BLOCKS), :] + sigma * (bounds[...] - (2.0 * image - img[...])), 0.0
        )
        img[...] = image
        return 0

    lax.fori_loop(0, ITERS, iteration, 0)

    violation_out(ITERS - 1)

    hot = jnp.broadcast_to(dst_ref[...], (BLOCKS, BLOCKS)) == iota((BLOCKS, BLOCKS), 0)
    ordered = dot(hot.astype(F32), dual[pl.ds(0, BLOCKS), :], exact=True)
    for i in range(BLOCKS):
        dsnd[i] = ordered[i : i + 1]
    drcv[me] = dsnd[me]
    to_plane(lambda i: dsnd.at[i], drcv.at[me], ds_sem, dr_sem)
    violation_plane(ITERS - 1)
    await_bytes(drcv.at[pl.ds(0, PLANE - 1)], dr_sem)
    dual_out = pltpu.make_async_copy(drcv, do_ref, last_sem.at[0])
    dual_out.start()
    new_weight(ITERS - 1)
    weight_out = pltpu.make_async_copy(wgt.at[pl.ds(0, 8), :], wo_ref, last_sem.at[1])
    weight_out.start()

    def drain(it, _):
        for j in range(CH):
            await_bytes(snd.at[it, j, pl.ds(0, PLANE - 1)], snd_sem.at[it, j])
            await_bytes(grad.at[it, j, pl.ds(0, PLANE - 1)], gs_sem.at[it, j])
            await_bytes(zrcv.at[it, j, pl.ds(0, ZN - 1)], zsnd_sem.at[it, j])

        await_bytes(vrcv.at[it, pl.ds(0, PLANE - 1)], vs_sem.at[it])
        await_bytes(vzrcv.at[it, pl.ds(0, ZN - 1)], vzs_sem.at[it])
        return 0

    lax.fori_loop(0, ITERS, drain, 0)
    await_bytes(dsnd.at[pl.ds(0, PLANE - 1)], ds_sem)
    pltpu.make_async_copy(x, xo_ref, out_sem).wait()
    dual_out.wait()
    weight_out.wait()


def hand_over(x_in, dual_in, weight_in, x_out, dual_out, weight_out, x, dual, weight, one, sem):
    part = NCB * CB // 4
    ins, outs = [], []
    for n in range(4):
        at = pl.ds(part * n, part)
        ins.append(pltpu.make_async_copy(x_in.at[at], x.at[at], sem.at[n]))
        outs.append(pltpu.make_async_copy(x.at[at], x_out.at[at], sem.at[6 + n]))
    ins.append(pltpu.make_async_copy(dual_in, dual, sem.at[4]))
    outs.append(pltpu.make_async_copy(dual, dual_out, sem.at[10]))
    last_in = pltpu.make_async_copy(weight_in, weight, sem.at[5])
    last_out = pltpu.make_async_copy(one, weight_out, sem.at[11])
    last_in.start()
    for copy in ins:
        copy.start()
    last_in.wait()
    one[0] = weight[0, 0]
    last_out.start()
    for copy, after in zip(ins, outs):
        copy.wait()
        after.start()
    for copy in outs:
        copy.wait()
    last_out.wait()


def per_device(tiles, col, counts, dest, bounds, dual0, primal, cost, upper):
    anywhere = pl.BlockSpec(memory_space=pl.ANY)
    dma = pltpu.SemaphoreType.DMA
    flat = (NCB * CB // TR, TR)
    x_out, dual_out, weight = pl.pallas_call(
        kernel,
        out_shape=(
            jax.ShapeDtypeStruct(flat, F32),
            jax.ShapeDtypeStruct((BLOCKS, 1, TR), F32),
            jax.ShapeDtypeStruct((8, TR), F32),
        ),
        in_specs=[anywhere] * 9,
        out_specs=(anywhere, anywhere, anywhere),
        scratch_shapes=[
            pltpu.VMEM((1, SLOTS), jnp.int32),
            pltpu.VMEM((1, BLOCKS), jnp.int32),
            pltpu.VMEM((1, BLOCKS), jnp.int32),
            pltpu.VMEM((BLOCKS, TR), BF16),
            pltpu.VMEM((BLOCKS, TR), BF16),
            pltpu.VMEM((CH, SLOTS, TR, LANES), BF16),
            pltpu.VMEM(flat, F32),
            pltpu.VMEM(flat, F32),
            pltpu.VMEM(flat, F32),
            pltpu.VMEM((CH, NCB, LANES), BF16),
            pltpu.VMEM((NCB, TR), BF16),
            pltpu.VMEM((TR, NCB), BF16),
            pltpu.VMEM((BLOCKS, 2 * TR), BF16),
            pltpu.VMEM((TR, TR), BF16),
            pltpu.VMEM((NG, GROUP, GROUP * TR), BF16),
            pltpu.VMEM((TR, LANES), F32),
            pltpu.VMEM((TR, TR), F32),
            pltpu.VMEM((TR, LANES), BF16),
            pltpu.VMEM((TR, LANES), F32),
            pltpu.VMEM((TR, TR), F32),
            pltpu.VMEM((SLOTS - CMAT, TR, TR), F32),
            pltpu.VMEM((BLOCKS, TR), F32),
            pltpu.VMEM((TR, TR), F32),
            pltpu.VMEM((16, TR), F32),
            pltpu.VMEM((ITERS, CH, PLANE, 16, TR), BF16),
            pltpu.VMEM((ITERS, CH, PLANE, 16, TR), BF16),
            pltpu.VMEM((ITERS, CH, 16, TR), F32),
            pltpu.VMEM((ITERS, CH, ZN, 16, TR), F32),
            pltpu.VMEM((ITERS, CH, PLANE, 16, TR), BF16),
            pltpu.VMEM((ITERS, 1, TR), F32),
            pltpu.VMEM((ITERS, PLANE, 1, TR), F32),
            pltpu.VMEM((ITERS, 1, TR), F32),
            pltpu.VMEM((ITERS, ZN, 1, TR), F32),
            pltpu.VMEM((BLOCKS, 1, TR), F32),
            pltpu.VMEM((BLOCKS, 1, TR), F32),
            pltpu.VMEM((BLOCKS, TR), F32),
            dma((CH,)),
            dma((3,)),
            dma((5,)),
            dma,
            dma((2,)),
            dma((ITERS, CH)),
            dma((ITERS, CH)),
            dma((ITERS, CH)),
            dma((ITERS, CH)),
            dma((ITERS, CH)),
            dma((ITERS, CH)),
            dma((ITERS,)),
            dma((ITERS,)),
            dma((ITERS,)),
            dma((ITERS,)),
            dma,
            dma,
        ],
        compiler_params=pltpu.CompilerParams(
            collective_id=0, has_side_effects=True, vmem_limit_bytes=60 * 1024 * 1024
        ),
    )(
        tiles,
        col.reshape(1, SLOTS),
        counts.reshape(1, BLOCKS),
        dest.reshape(1, BLOCKS),
        bounds.reshape(BLOCKS, TR),
        dual0.reshape(BLOCKS, TR),
        primal.reshape(flat),
        cost.reshape(flat),
        upper.reshape(flat),
    )
    return pl.pallas_call(
        hand_over,
        out_shape=(
            jax.ShapeDtypeStruct((NCB * CB,), F32),
            jax.ShapeDtypeStruct((BLOCKS * TR,), F32),
            jax.ShapeDtypeStruct((1,), F32),
        ),
        in_specs=[anywhere] * 3,
        out_specs=(anywhere, anywhere, anywhere),
        scratch_shapes=[
            pltpu.VMEM((NCB * CB,), F32),
            pltpu.VMEM((BLOCKS * TR,), F32),
            pltpu.VMEM((8, TR), F32),
            pltpu.SMEM((1,), F32),
            dma((12,)),
        ],
    )(x_out.reshape(-1), dual_out.reshape(-1), weight)


def solution(mesh):
    split, whole = P(GRP_DEV), P()
    return jax.shard_map(
        per_device,
        mesh=mesh,
        in_specs=(P(GRP_DEV, None, None), split, split, split, split, split, whole, whole, whole),
        out_specs=(whole, split, whole),
        check_vma=False,
    )
```

```python
import jax
import jax.numpy as jnp
from jax import lax
from jax.experimental import pallas as pl
from jax.experimental.pallas import tpu as pltpu
from jax.sharding import PartitionSpec as P

MESH = pl.DeviceIdType.MESH
GRP_DEV = ("grp", "dev")

NCB = 256
CB = 1024
TR = 128
SLOTS = 80
BLOCKS = 32
ITERS = 3
CH = 4
LANES = CB // CH
GROUP = 16
NG = SLOTS // GROUP
VSLOTS = 40
RGROUP = 8
CMAT = 64
PLANE = 32
ZN = 4
STEP = 0.3

F32 = jnp.float32
BF16 = jnp.bfloat16


def iota(shape, dim):
    return lax.broadcasted_iota(jnp.int32, shape, dim)


def dot(a, b, dims=((1,), (0,)), exact=False):
    return lax.dot_general(
        a,
        b,
        (dims, ((), ())),
        precision=lax.Precision.HIGHEST if exact else None,
        preferred_element_type=F32,
    )


def kernel(
    tiles_hbm,
    col_hbm,
    cnt_hbm,
    dst_hbm,
    bnd_hbm,
    dual0_hbm,
    x_hbm,
    c_hbm,
    u_hbm,
    xo_ref,
    do_ref,
    wo_ref,
    col_ref,
    cnt_ref,
    dst_ref,
    bnd_ref,
    dual0_ref,
    tiles,
    x,
    cost,
    upper,
    xtab,
    cmat,
    ctmat,
    omat,
    otmat,
    bd,
    prod,
    macc,
    vsel,
    vrow,
    wcol,
    wide,
    img,
    dual,
    wgt,
    snd,
    rcv,
    zsnd,
    zrcv,
    grad,
    vsnd,
    vrcv,
    vzsnd,
    vzrcv,
    dsnd,
    drcv,
    bounds,
    tile_sem,
    vec_sem,
    small_sem,
    out_sem,
    last_sem,
    snd_sem,
    rcv_sem,
    zsnd_sem,
    zrcv_sem,
    gs_sem,
    gr_sem,
    vs_sem,
    vr_sem,
    vzs_sem,
    vzr_sem,
    ds_sem,
    dr_sem,
):
    z = lax.axis_index("grp")
    me = lax.axis_index("dev")

    vec_copies = [
        pltpu.make_async_copy(h, v, vec_sem.at[n])
        for n, (h, v) in enumerate(((x_hbm, x), (c_hbm, cost), (u_hbm, upper)))
    ]

    def tile_copy(j):
        return pltpu.make_async_copy(
            tiles_hbm.at[:, :, pl.ds(LANES * j, LANES)], tiles.at[j], tile_sem.at[j]
        )

    small = (
        (col_hbm, col_ref),
        (cnt_hbm, cnt_ref),
        (dst_hbm, dst_ref),
        (bnd_hbm, bnd_ref),
        (dual0_hbm, dual0_ref),
    )
    small = [pltpu.make_async_copy(h, v, small_sem.at[n]) for n, (h, v) in enumerate(small)]
    for copy in small:
        copy.start()
    tile_copy(0).start()
    vec_copies[0].start()

    along = [8 * lax.rem(me // 8 + k, 4) for k in range(4)]
    across = [2 * lax.rem(me // 2 + k, 4) for k in range(4)]
    cores = [lax.rem(me + k, 2) for k in range(2)]
    peers = [
        along[a] + across[b] + cores[c]
        for hops in (4, 3, 2, 1, 0)
        for a in range(4)
        for b in range(4)
        for c in range(2)
        if min(a, 4 - a) + min(b, 4 - b) == hops and (a, b, c) != (0, 0, 0)
    ]

    barrier = pltpu.get_barrier_semaphore()
    for peer in peers:
        pl.semaphore_signal(barrier, inc=1, device_id=(z, peer), device_id_type=MESH)
    for k in (2, 1, 3):
        pl.semaphore_signal(
            barrier, inc=1, device_id=(lax.rem(z + k, ZN), me), device_id_type=MESH
        )

    def to_plane(src, dst, ssem, rsem):
        for peer in peers:
            pltpu.make_async_remote_copy(
                src_ref=src(peer),
                dst_ref=dst,
                send_sem=ssem,
                recv_sem=rsem,
                device_id=(z, peer),
                device_id_type=MESH,
            ).start()

    def to_z(src, dst, ssem, rsem, peer_z):
        pltpu.make_async_remote_copy(
            src_ref=src,
            dst_ref=dst,
            send_sem=ssem,
            recv_sem=rsem,
            device_id=(peer_z, me),
            device_id_type=MESH,
        ).start()

    def await_bytes(ref, sem):
        pltpu.make_async_copy(ref, ref, sem).wait()

    for copy in small:
        copy.wait()
    cols = jnp.broadcast_to(col_ref[...], (NCB, SLOTS))
    onehot = (cols == iota((NCB, SLOTS), 0)).astype(F32)
    onehot = jnp.concatenate([onehot, jnp.zeros((NCB, TR - SLOTS), F32)], axis=1)
    cmat[...] = onehot.astype(BF16)
    ctmat[...] = onehot.T.astype(BF16)
    counts = jnp.broadcast_to(cnt_ref[...], (TR, BLOCKS)).astype(F32)
    below = (iota((BLOCKS, BLOCKS), 1) < iota((BLOCKS, BLOCKS), 0)).astype(F32)
    upto = (iota((BLOCKS, BLOCKS), 1) <= iota((BLOCKS, BLOCKS), 0)).astype(F32)
    starts = dot(below, counts, ((1,), (1,)))
    ends = dot(upto, counts, ((1,), (1,)))
    slot = iota((BLOCKS, TR), 1).astype(F32)
    owner = jnp.where((starts <= slot) & (slot < ends), 1.0, 0.0)
    omat[:, :TR] = owner.astype(BF16)
    omat[:, TR:] = owner.astype(BF16)
    owner = jnp.concatenate([owner, jnp.zeros((TR - BLOCKS, TR), F32)], axis=0)
    otmat[...] = owner.T.astype(BF16)
    prod[...] = jnp.zeros_like(prod)
    macc[...] = jnp.zeros_like(macc)
    wgt[...] = jnp.ones_like(wgt)
    dual[...] = jnp.zeros_like(dual)
    dual[pl.ds(0, BLOCKS), :] = dual0_ref[...].astype(F32)
    bounds[...] = bnd_ref[...].astype(F32)

    def pieces(j, body, start):
        def row(p, carry):
            for c in range(2):
                at = pl.ds(TR * p + 2 * j + c, 16, stride=8)
                carry = body(p, c, at, carry)
            return carry

        return lax.fori_loop(0, 16, row, start, unroll=8)

    def table(j, p, c, value):
        xtab[j, pl.ds(pl.multiple_of(16 * p, 16), 16), pl.ds(TR * c, TR)] = value.astype(BF16)

    def first_table(j):
        def fill(p, c, at, carry):
            table(j, p, c, x[at, :])
            return carry

        pieces(j, fill, 0)

    def columns(it, j, first):
        def by_matmul(g):
            at = pl.ds(GROUP * g, GROUP)
            prod[at, :] = dot(bd[g], tiles[j, at].reshape(GROUP * TR, LANES))

        def by_vector(s):
            if first:
                spot = wcol[:, s : s + 1]
                scale = jnp.broadcast_to(spot, (TR, TR))
                wide[s - CMAT] = scale
            else:
                scale = wide[s - CMAT]
            part = tiles[j, s].astype(F32)
            for c in range(2):
                lanes = pl.ds(TR * c, TR)
                some = part[:, TR * c : TR * (c + 1)] * scale
                prod[pl.ds(s, 1), lanes] = jnp.sum(some, axis=0, keepdims=True)

        left = list(range(CMAT, SLOTS))
        groups = CMAT // GROUP
        share = -(-len(left) // groups)
        for g in range(groups):
            by_matmul(g)
            for s in left[share * g : share * (g + 1)]:
                by_vector(s)
        full = prod[...]
        high = full.astype(BF16)
        low = (full - high.astype(F32)).astype(BF16)
        total = dot(cmat[...], high) + dot(cmat[...], low)
        total = total.astype(BF16)
        for c in range(2):
            snd[it, j, pl.ds(16 * c, 16)] = total[:, TR * c : TR * (c + 1)].reshape(16, 16, TR)

    def columns_out(it, j):
        to_plane(lambda i: snd.at[it, j, i], rcv.at[it, j, me], snd_sem.at[it, j], rcv_sem.at[it, j])

    def rows(j):
        picked = dot(ctmat[...], xtab[j])
        vsel[...] = picked.astype(BF16)
        vrow[...] = picked
        lane = iota((TR, TR), 1)

        def by_matmul(g, merged):
            block = tiles[j, pl.ds(RGROUP * g, RGROUP)].reshape(RGROUP * TR, LANES)
            out = dot(block, vsel[...], ((1,), (1,)))
            for k in range(RGROUP):
                merged = jnp.where(lane == RGROUP * g + k, out[TR * k : TR * (k + 1)], merged)
            return merged

        def by_vector(s, merged):
            part = tiles[j, s].astype(F32) * vrow[pl.ds(s, 1), :]
            part = part[:, :TR] + part[:, TR:]
            return jnp.where(lane == s, jnp.sum(part, axis=1, keepdims=True), merged)

        merged = jnp.zeros((TR, TR), F32)
        left = list(range(SLOTS - VSLOTS, SLOTS))
        groups = (SLOTS - VSLOTS) // RGROUP
        share = -(-VSLOTS // groups)
        for g in range(groups):
            merged = by_matmul(g, merged)
            for s in left[share * g : share * (g + 1)]:
                merged = by_vector(s, merged)
        macc[...] += merged

    def rows_done():
        full = macc[...]
        high = full.astype(BF16)
        low = (full - high.astype(F32)).astype(BF16)
        out = dot(omat[...], jnp.concatenate([high, low], axis=1), ((1,), (1,)))
        macc[...] = jnp.zeros_like(macc)
        return out

    def plane_sum(it, j):
        rcv[it, j, me] = snd[it, j, me]
        await_bytes(rcv.at[it, j, pl.ds(0, PLANE - 1)], rcv_sem.at[it, j])
        total = rcv[it, j, 0].astype(F32)
        for i in range(1, PLANE):
            total += rcv[it, j, i].astype(F32)

        zsnd[it, j] = total
        zrcv[it, j, z] = total
        for k in (2, 1, 3):
            to_z(
                zsnd.at[it, j],
                zrcv.at[it, j, z],
                zsnd_sem.at[it, j],
                zrcv_sem.at[it, j],
                lax.rem(z + k, ZN),
            )

    def spread(it, j):
        await_bytes(zrcv.at[it, j, pl.ds(0, ZN - 1)], zrcv_sem.at[it, j])
        total = zrcv[it, j, 0] + zrcv[it, j, 1] + zrcv[it, j, 2] + zrcv[it, j, 3]
        grad[it, j, me] = total.astype(BF16)
        to_plane(
            lambda i: grad.at[it, j, me], grad.at[it, j, me], gs_sem.at[it, j], gr_sem.at[it, j]
        )

    def violation_in(it, violated):
        part = violated[0:8] + violated[8:16] + violated[16:24] + violated[24:32]
        part = jnp.sum(part, axis=0, keepdims=True)
        vsnd[it] = part
        vrcv[it, me] = part

    def violation_out(it):
        to_plane(lambda i: vsnd.at[it], vrcv.at[it, me], vs_sem.at[it], vr_sem.at[it])

    def violation_plane(it):
        await_bytes(vrcv.at[it, pl.ds(0, PLANE - 1)], vr_sem.at[it])
        total = vrcv[it, 0]
        for i in range(1, PLANE):
            total += vrcv[it, i]
        vzsnd[it] = total
        vzrcv[it, z] = total
        for k in (2, 1, 3):
            to_z(
                vzsnd.at[it],
                vzrcv.at[it, z],
                vzs_sem.at[it],
                vzr_sem.at[it],
                lax.rem(z + k, ZN),
            )

    def new_weight(it):
        await_bytes(vzrcv.at[it, pl.ds(0, ZN - 1)], vzr_sem.at[it])
        total = vzrcv[it, 0] + vzrcv[it, 1] + vzrcv[it, 2] + vzrcv[it, 3]
        violation = jnp.sum(total, axis=1, keepdims=True)
        change = wgt[pl.ds(8, 8), :]
        ratio = (jnp.broadcast_to(violation, (8, TR)) + 1e-6) / (change + 1e-6)
        wgt[pl.ds(0, 8), :] = jnp.sqrt(wgt[pl.ds(0, 8), :] * jnp.sqrt(ratio))

    def update(it, j, tau, moved):
        def piece(p, c, at, carry):
            old = x[at, :]
            slope = grad[it, j, 16 * c + p].astype(F32)
            new = jnp.minimum(jnp.maximum(old - tau * (cost[at, :] - slope), 0.0), upper[at, :])
            x[at, :] = new
            table(j, p, c, new)
            return carry + (new - old) * (new - old)

        return pieces(j, piece, moved)

    def iteration(it, _):
        chosen = dot(otmat[...], dual[...].astype(BF16))
        line = iota((GROUP, TR), 0)
        wcol[...] = chosen.T
        for g in range(CMAT // GROUP):
            part = chosen[GROUP * g : GROUP * (g + 1)]
            for k in range(GROUP):
                bd[g, :, pl.ds(TR * k, TR)] = jnp.where(line == k, part, 0.0).astype(BF16)
        @pl.when(it == 0)
        def _():
            tile_copy(1).start()
            tile_copy(0).wait()
            for j in range(2, CH):
                tile_copy(j).start()
            vec_copies[1].start()
            vec_copies[2].start()

        columns(it, 0, True)

        @pl.when(it == 0)
        def _():
            pl.semaphore_wait(barrier, PLANE - 1 + ZN - 1)

        columns_out(it, 0)

        @pl.when(it == 0)
        def _():
            vec_copies[0].wait()
            first_table(0)

        def later(j, _):
            @pl.when(it == 0)
            def _():
                first_table(j)
                tile_copy(j).wait()

            columns(it, j, False)
            columns_out(it, j)
            return 0

        lax.fori_loop(1, CH, later, 0)

        def early_rows(j):
            @pl.when(it == 0)
            def _():
                rows(j)

        @pl.when(it > 0)
        def _():
            violation_out(it - 1)

        plane_sum(it, 0)
        early_rows(0)
        plane_sum(it, 1)

        @pl.when(it == 0)
        def _():
            spread(it, 0)
            plane_sum(it, 2)
            rows(1)

        @pl.when(it > 0)
        def _():
            plane_sum(it, 2)
            spread(it, 0)
            plane_sum(it, 3)

        spread(it, 1)

        @pl.when(it == 0)
        def _():
            plane_sum(it, 3)
            rows(2)

        @pl.when(it > 0)
        def _():
            violation_plane(it - 1)

        spread(it, 2)
        early_rows(3)
        spread(it, 3)

        @pl.when(it == 0)
        def _():
            img[...] = rows_done()
            vec_copies[1].wait()
            vec_copies[2].wait()

        @pl.when(it > 0)
        def _():
            new_weight(it - 1)

        weight = wgt[pl.ds(0, 1), :]
        tau = STEP / weight
        sigma = STEP * weight
        moved = jnp.zeros((16, TR), F32)
        def step(j, moved):
            await_bytes(grad.at[it, j, pl.ds(0, PLANE - 1)], gr_sem.at[it, j])
            moved = update(it, j, tau, moved)
            rows(j)
            return moved

        moved = lax.fori_loop(0, CH, step, moved)

        @pl.when(it == ITERS - 1)
        def _():
            pltpu.make_async_copy(x, xo_ref, out_sem).start()

        change = jnp.sum(jnp.sum(moved, axis=0, keepdims=True), axis=1, keepdims=True)
        wgt[pl.ds(8, 8), :] = jnp.broadcast_to(change, (8, TR))
        image = rows_done()
        violated = jnp.maximum(bounds[...] - image, 0.0)
        violation_in(it, violated * violated)
        dual[pl.ds(0, BLOCKS), :] = jnp.maximum(
            dual[pl.ds(0, BLOCKS), :] + sigma * (bounds[...] - (2.0 * image - img[...])), 0.0
        )
        img[...] = image
        return 0

    lax.fori_loop(0, ITERS, iteration, 0)

    violation_out(ITERS - 1)

    hot = jnp.broadcast_to(dst_ref[...], (BLOCKS, BLOCKS)) == iota((BLOCKS, BLOCKS), 0)
    ordered = dot(hot.astype(F32), dual[pl.ds(0, BLOCKS), :], exact=True)
    for i in range(BLOCKS):
        dsnd[i] = ordered[i : i + 1]
    drcv[me] = dsnd[me]
    to_plane(lambda i: dsnd.at[i], drcv.at[me], ds_sem, dr_sem)
    violation_plane(ITERS - 1)
    await_bytes(drcv.at[pl.ds(0, PLANE - 1)], dr_sem)
    dual_out = pltpu.make_async_copy(drcv, do_ref, last_sem.at[0])
    dual_out.start()
    new_weight(ITERS - 1)
    weight_out = pltpu.make_async_copy(wgt.at[pl.ds(0, 8), :], wo_ref, last_sem.at[1])
    weight_out.start()

    def drain(it, _):
        for j in range(CH):
            await_bytes(snd.at[it, j, pl.ds(0, PLANE - 1)], snd_sem.at[it, j])
            await_bytes(grad.at[it, j, pl.ds(0, PLANE - 1)], gs_sem.at[it, j])
            await_bytes(zrcv.at[it, j, pl.ds(0, ZN - 1)], zsnd_sem.at[it, j])

        await_bytes(vrcv.at[it, pl.ds(0, PLANE - 1)], vs_sem.at[it])
        await_bytes(vzrcv.at[it, pl.ds(0, ZN - 1)], vzs_sem.at[it])
        return 0

    lax.fori_loop(0, ITERS, drain, 0)
    await_bytes(dsnd.at[pl.ds(0, PLANE - 1)], ds_sem)
    pltpu.make_async_copy(x, xo_ref, out_sem).wait()
    dual_out.wait()
    weight_out.wait()


def hand_over(x_in, dual_in, weight_in, x_out, dual_out, weight_out, x, dual, weight, one, sem):
    part = NCB * CB // 4
    ins, outs = [], []
    for n in range(4):
        at = pl.ds(part * n, part)
        ins.append(pltpu.make_async_copy(x_in.at[at], x.at[at], sem.at[n]))
        outs.append(pltpu.make_async_copy(x.at[at], x_out.at[at], sem.at[6 + n]))
    ins.append(pltpu.make_async_copy(dual_in, dual, sem.at[4]))
    outs.append(pltpu.make_async_copy(dual, dual_out, sem.at[10]))
    last_in = pltpu.make_async_copy(weight_in, weight, sem.at[5])
    last_out = pltpu.make_async_copy(one, weight_out, sem.at[11])
    last_in.start()
    for copy in ins:
        copy.start()
    last_in.wait()
    one[0] = weight[0, 0]
    last_out.start()
    for copy, after in zip(ins, outs):
        copy.wait()
        after.start()
    for copy in outs:
        copy.wait()
    last_out.wait()


def per_device(tiles, col, counts, dest, bounds, dual0, primal, cost, upper):
    anywhere = pl.BlockSpec(memory_space=pl.ANY)
    dma = pltpu.SemaphoreType.DMA
    flat = (NCB * CB // TR, TR)
    x_out, dual_out, weight = pl.pallas_call(
        kernel,
        out_shape=(
            jax.ShapeDtypeStruct(flat, F32),
            jax.ShapeDtypeStruct((BLOCKS, 1, TR), F32),
            jax.ShapeDtypeStruct((8, TR), F32),
        ),
        in_specs=[anywhere] * 9,
        out_specs=(anywhere, anywhere, anywhere),
        scratch_shapes=[
            pltpu.VMEM((1, SLOTS), jnp.int32),
            pltpu.VMEM((1, BLOCKS), jnp.int32),
            pltpu.VMEM((1, BLOCKS), jnp.int32),
            pltpu.VMEM((BLOCKS, TR), BF16),
            pltpu.VMEM((BLOCKS, TR), BF16),
            pltpu.VMEM((CH, SLOTS, TR, LANES), BF16),
            pltpu.VMEM(flat, F32),
            pltpu.VMEM(flat, F32),
            pltpu.VMEM(flat, F32),
            pltpu.VMEM((CH, NCB, LANES), BF16),
            pltpu.VMEM((NCB, TR), BF16),
            pltpu.VMEM((TR, NCB), BF16),
            pltpu.VMEM((BLOCKS, 2 * TR), BF16),
            pltpu.VMEM((TR, TR), BF16),
            pltpu.VMEM((NG, GROUP, GROUP * TR), BF16),
            pltpu.VMEM((TR, LANES), F32),
            pltpu.VMEM((TR, TR), F32),
            pltpu.VMEM((TR, LANES), BF16),
            pltpu.VMEM((TR, LANES), F32),
            pltpu.VMEM((TR, TR), F32),
            pltpu.VMEM((SLOTS - CMAT, TR, TR), F32),
            pltpu.VMEM((BLOCKS, TR), F32),
            pltpu.VMEM((TR, TR), F32),
            pltpu.VMEM((16, TR), F32),
            pltpu.VMEM((ITERS, CH, PLANE, 16, TR), BF16),
            pltpu.VMEM((ITERS, CH, PLANE, 16, TR), BF16),
            pltpu.VMEM((ITERS, CH, 16, TR), F32),
            pltpu.VMEM((ITERS, CH, ZN, 16, TR), F32),
            pltpu.VMEM((ITERS, CH, PLANE, 16, TR), BF16),
            pltpu.VMEM((ITERS, 1, TR), F32),
            pltpu.VMEM((ITERS, PLANE, 1, TR), F32),
            pltpu.VMEM((ITERS, 1, TR), F32),
            pltpu.VMEM((ITERS, ZN, 1, TR), F32),
            pltpu.VMEM((BLOCKS, 1, TR), F32),
            pltpu.VMEM((BLOCKS, 1, TR), F32),
            pltpu.VMEM((BLOCKS, TR), F32),
            dma((CH,)),
            dma((3,)),
            dma((5,)),
            dma,
            dma((2,)),
            dma((ITERS, CH)),
            dma((ITERS, CH)),
            dma((ITERS, CH)),
            dma((ITERS, CH)),
            dma((ITERS, CH)),
            dma((ITERS, CH)),
            dma((ITERS,)),
            dma((ITERS,)),
            dma((ITERS,)),
            dma((ITERS,)),
            dma,
            dma,
        ],
        compiler_params=pltpu.CompilerParams(
            collective_id=0, has_side_effects=True, vmem_limit_bytes=60 * 1024 * 1024
        ),
    )(
        tiles,
        col.reshape(1, SLOTS),
        counts.reshape(1, BLOCKS),
        dest.reshape(1, BLOCKS),
        bounds.reshape(BLOCKS, TR),
        dual0.reshape(BLOCKS, TR),
        primal.reshape(flat),
        cost.reshape(flat),
        upper.reshape(flat),
    )
    return pl.pallas_call(
        hand_over,
        out_shape=(
            jax.ShapeDtypeStruct((NCB * CB,), F32),
            jax.ShapeDtypeStruct((BLOCKS * TR,), F32),
            jax.ShapeDtypeStruct((1,), F32),
        ),
        in_specs=[anywhere] * 3,
        out_specs=(anywhere, anywhere, anywhere),
        scratch_shapes=[
            pltpu.VMEM((NCB * CB,), F32),
            pltpu.VMEM((BLOCKS * TR,), F32),
            pltpu.VMEM((8, TR), F32),
            pltpu.SMEM((1,), F32),
            dma((12,)),
        ],
    )(x_out.reshape(-1), dual_out.reshape(-1), weight)


def solution(mesh):
    split, whole = P(GRP_DEV), P()
    return jax.shard_map(
        per_device,
        mesh=mesh,
        in_specs=(P(GRP_DEV, None, None), split, split, split, split, split, whole, whole, whole),
        out_specs=(whole, split, whole),
        check_vma=False,
    )
```
